128 devices in a mesh: dp: 32 (over x, y, z_hi), pipe: 4 (over z_lo, core).
Axes of the slice: x: 4, y: 4, z: 4 (z_hi: 2, z_lo: 2; z = z_hi * 2 + z_lo), core: 2. Of those that a mesh axis runs over, the one named last changes fastest.
Arguments:
- master: float32 [4, 512, 8192], P('pipe', 'dp'), may hold values from -0.12 to 0.12
- moment1: float32 [4, 512, 8192], P('pipe', 'dp'), may hold values from -3 to 3
- moment2: float32 [4, 512, 8192], P('pipe', 'dp'), may hold values from 0.25 to 4.5
- quant_grad: bfloat16 [4, 512, 8192], P('pipe', 'dp'), may hold values from -120 to 120
- grad_exponent: int32 [4, 512], P('pipe', 'dp'), may hold values from -3 to 2
- replica_params: bfloat16 [4, 32, 512, 8192], P('pipe', 'dp'), as said below
- failed: int32 [4, 2], replicated, may hold values from 0 to 31, as said below
- dest: int32 [4, 512], replicated, may hold values from 0 to 511, as said below
Outputs:
- new_master: float32 [4, 512, 8192], P('pipe', 'dp')
- new_moment1: float32 [4, 512, 8192], P('pipe', 'dp')
- new_moment2: float32 [4, 512, 8192], P('pipe', 'dp')
The draws below stay inside these ranges and needn't reach their ends.
Inputs may be any that keep to these rules, and one draw needn't show every extreme that they name: `failed`: each group lists 2 distinct ranks; group 0 lists ranks 1 and 16; in every other group some rows of the first listed rank have new positions among the rows of the second listed rank (new position // 16). `dest`: each group's row is a permutation of its rows; the 16 rows of one rank (old rows r * 16 to r * 16 + 15) land in at most 1 row of any one rank's new rows (new position // 16), and some pair of ranks reaches 1 in every group. `replica_params`: within a group the copies of ranks not listed in failed are equal; the copies of listed ranks are zero.
All inputs are finite; a program needn't handle non-finite values.
Results may differ from the reference program's by a relative error of at most 0.0003.
Values may be sent and summed in bfloat16 or wider, within the bound.
A program may use at most 64 MiB of HBM per device.

```python
import math
import jax
import jax.numpy as jnp
from jax import lax

D = 8192
K = 16
FMAX = 2
STEP = 20
RANKS = 32
GROUPS = 4
GROUP_ROWS = 512
CAP = 1


def group_dest(group_key):
    per_layer = K // CAP
    first_key = jax.random.fold_in(group_key, 1)
    base_perm = jax.random.permutation(first_key, RANKS)
    layer_perms = []
    layer_offsets = []
    for layer in range(CAP):
        rest_perm = 1 + jax.random.permutation(jax.random.fold_in(group_key, 100 + layer), RANKS - 1)
        mixer = jnp.concatenate([jnp.zeros((1,), jnp.int32), rest_perm.astype(jnp.int32)])
        layer_perms.append(base_perm[mixer])
        offset_pick = 1 + jax.random.permutation(jax.random.fold_in(group_key, 200 + layer), RANKS - 1)
        layer_offsets.append(jnp.concatenate([jnp.zeros((1,), jnp.int32), offset_pick[:per_layer - 1].astype(jnp.int32)]))
    taus = jnp.stack(layer_perms)
    offsets = jnp.stack(layer_offsets)
    targets = ((taus.T[:, :, None] + offsets[None, :, :]) % RANKS).reshape(RANKS, K)
    row_keys = jax.random.split(jax.random.fold_in(group_key, 3), RANKS)
    row_perm = jax.vmap(lambda row_key: jax.random.permutation(row_key, K))(row_keys)
    target_rows = jnp.take_along_axis(targets, row_perm, axis=1).reshape(-1)
    scores = jax.random.permutation(jax.random.fold_in(group_key, 4), GROUP_ROWS)
    same_target = target_rows[None, :] == target_rows[:, None]
    before = scores[None, :] < scores[:, None]
    slot_index = jnp.sum((same_target & before).astype(jnp.int32), axis=1)
    return (target_rows * K + slot_index).astype(jnp.int32)


def group_failed(group_key, dest_row, group_index):
    order_scores = jax.random.permutation(jax.random.fold_in(group_key, 5), RANKS).astype(jnp.int32)
    pick_scores = jax.random.permutation(jax.random.fold_in(group_key, 6), RANKS).astype(jnp.int32)
    first_rank = jnp.argmax(order_scores).astype(jnp.int32)
    old_rank = (jnp.arange(GROUP_ROWS, dtype=jnp.int32) // K).astype(jnp.int32)
    new_rank = (dest_row // K).astype(jnp.int32)
    from_first = old_rank == first_rank
    rank_ids = jnp.arange(RANKS, dtype=jnp.int32)
    reach = jnp.any(from_first[None, :] & (new_rank[None, :] == rank_ids[:, None]), axis=1)
    ranking = jnp.where(rank_ids == first_rank, 3 * RANKS, jnp.where(reach, 2 * RANKS + pick_scores, pick_scores))
    drawn = lax.top_k(ranking.astype(jnp.int32), FMAX)[1].astype(jnp.int32)
    fixed = jnp.array([1, RANKS // 2], dtype=jnp.int32)
    return jnp.where(group_index == 0, fixed, drawn).astype(jnp.int32)


def group_keys_of(key):
    return jax.random.split(jax.random.fold_in(key, 21), GROUPS)


def draw_dest(key, part):
    return jax.vmap(group_dest)(group_keys_of(key))


def failed_ranks(key):
    group_keys = group_keys_of(key)
    dests = jax.vmap(group_dest)(group_keys)
    return jax.vmap(group_failed)(group_keys, dests, jnp.arange(GROUPS, dtype=jnp.int32)).astype(jnp.int32)


def draw_failed(key, part):
    return failed_ranks(key)


def draw_replica_params(key, part):
    lost_ranks = failed_ranks(key)
    base_rows = jax.random.normal(jax.random.fold_in(key, 12), (GROUPS, GROUP_ROWS, D), jnp.float32) * 0.02
    rank_ids = jnp.arange(RANKS, dtype=jnp.int32)
    is_failed = jnp.any(rank_ids[None, :, None] == lost_ranks[:, None, :], axis=2)
    return jnp.where(is_failed[:, :, None, None], jnp.float32(0.0), base_rows[:, None, :, :]).astype(jnp.bfloat16)


def draw_grad_exponent(key, part):
    base_exp = jax.random.randint(jax.random.fold_in(key, 30), (GROUPS, GROUP_ROWS), -3, 2)
    trend = 2 * (jnp.arange(GROUP_ROWS) // K) // RANKS
    return (base_exp + trend[None, :]).astype(jnp.int32)


def draw_quant_grad(key, part):
    noise = jnp.clip(jax.random.normal(jax.random.fold_in(key, 41), (GROUPS, GROUP_ROWS, D), jnp.float32), -5.0, 5.0)
    column_draw = jax.random.uniform(jax.random.fold_in(key, 42), (D,), jnp.float32)
    column_scale = jnp.exp(column_draw * math.log(10.0))
    return (noise * column_scale[None, None, :]).astype(jnp.bfloat16)


def draw_master(key, part):
    sub_key = jax.random.fold_in(key, 51)
    noise = jax.random.normal(jax.random.fold_in(sub_key, 3), (GROUPS, GROUP_ROWS, D), jnp.float32)
    return jnp.clip(noise, -6.0, 6.0) * 0.02


def draw_moment1(key, part):
    sub_key = jax.random.fold_in(key, 61)
    noise = jax.random.normal(jax.random.fold_in(sub_key, 3), (GROUPS, GROUP_ROWS, D), jnp.float32)
    return jnp.clip(noise, -6.0, 6.0) * 0.5


def draw_moment2(key, part):
    level_draw = jax.random.uniform(jax.random.fold_in(key, 71), (GROUPS, GROUP_ROWS, D), jnp.float32)
    return jnp.exp(math.log(0.25) + level_draw * math.log(16.0))


def setup_inputs(seed: int = 0) -> dict:
    keys = jax.random.split(jax.random.key(seed), 9)
    return {
        "master": draw_master(jax.random.fold_in(keys[8], 71), 0),
        "moment1": draw_moment1(jax.random.fold_in(keys[8], 71), 0),
        "moment2": draw_moment2(jax.random.fold_in(keys[8], 71), 0),
        "quant_grad": draw_quant_grad(jax.random.fold_in(keys[8], 71), 0),
        "grad_exponent": draw_grad_exponent(jax.random.fold_in(keys[8], 71), 0),
        "replica_params": draw_replica_params(jax.random.fold_in(keys[8], 71), 0),
        "failed": draw_failed(jax.random.fold_in(keys[8], 71), 0),
        "dest": draw_dest(jax.random.fold_in(keys[8], 71), 0),
    }


beta_one = 0.9
beta_two = 0.95
learn_rate = 0.00015
decay_rate = 0.1
adam_eps = 1e-08
clip_eps = 1e-06

def adam_step(weights, first, second, grads):
    first_new = beta_one * first + (1.0 - beta_one) * grads
    second_new = beta_two * second + (1.0 - beta_two) * grads * grads
    corr_one = 1.0 - beta_one ** STEP
    corr_two = 1.0 - beta_two ** STEP
    direction = first_new / corr_one / (jnp.sqrt(second_new / corr_two) + adam_eps) + decay_rate * weights
    return (weights - learn_rate * direction, first_new, second_new)

def reference(master, moment1, moment2, quant_grad, grad_exponent, replica_params, failed, dest):
    grad = quant_grad.astype(jnp.float32) * jnp.exp2(grad_exponent.astype(jnp.float32))[:, :, None]
    grad_total = jnp.sum(grad * grad)
    clip_scale = jnp.minimum(1.0, 1.0 / jnp.sqrt(grad_total / (GROUPS * GROUP_ROWS * D) + clip_eps))
    clipped = grad * clip_scale
    rank_ids = jnp.arange(RANKS, dtype=jnp.int32)
    is_alive = jnp.all(rank_ids[None, :, None] != failed[:, None, :], axis=2)
    root_rank = lax.optimization_barrier(jnp.min(jnp.where(is_alive, rank_ids[None, :], RANKS), axis=1)).astype(jnp.int32)
    copy_rows = replica_params[jnp.arange(GROUPS, dtype=jnp.int32), root_rank].astype(jnp.float32)
    row_rank = (jnp.arange(GROUP_ROWS, dtype=jnp.int32) // K).astype(jnp.int32)
    is_lost = jnp.any(row_rank[None, :, None] == failed[:, None, :], axis=2)[:, :, None]
    start_master = jnp.where(is_lost, copy_rows, master)
    start_first = jnp.where(is_lost, jnp.float32(0.0), moment1)
    start_second = jnp.where(is_lost, jnp.float32(0.0), moment2)
    w_next, m_next, v_next = adam_step(start_master, start_first, start_second, clipped)
    group_ids = jnp.broadcast_to(jnp.arange(GROUPS, dtype=jnp.int32)[:, None], dest.shape)
    out_master = jnp.zeros_like(w_next).at[group_ids, dest].set(w_next)
    out_first = jnp.zeros_like(m_next).at[group_ids, dest].set(m_next)
    out_second = jnp.zeros_like(v_next).at[group_ids, dest].set(v_next)
    return (out_master, out_first, out_second)
```

```python
import functools
import math

import jax
import jax.numpy as jnp
from jax import lax
from jax.experimental import pallas as pl
from jax.experimental.pallas import tpu as pltpu
from jax.sharding import PartitionSpec as P

STEP = 20

beta_one = 0.9
beta_two = 0.95
learn_rate = 0.00015
decay_rate = 0.1
adam_eps = 1e-08
clip_eps = 1e-06

corr_one = 1.0 - beta_one**STEP
corr_two = 1.0 - beta_two**STEP

MESH = pl.DeviceIdType.MESH
DP = 32
PIPE = 4
K = 16
D = 8192
HALF = D // 2
LANES = 128
W_COLS = HALF + 3 * LANES
CHUNKS = 4
CW = D // CHUNKS
STEP_COLS = 1024
TILES = STEP_COLS // LANES

SCALE_UNIT = 65536.0
TINY = 1e-30
LOG_LOW = -2.2
LOG_SPAN = 16.0
LOG_UNIT = 65535.0 / LOG_SPAN


def cols(step, width=STEP_COLS, base=0):
    return pl.ds(pl.multiple_of(base + step * width, LANES), width)


def tiled(scale):
    return jnp.concatenate([scale] * TILES, axis=1)


def fold(acc, op):
    out = acc[:, :LANES]
    for t in range(1, TILES):
        out = op(out, acc[:, t * LANES : (t + 1) * LANES])
    return out


def scale_code(scale):
    return jnp.ceil(jnp.log2(jnp.maximum(scale, TINY)) * SCALE_UNIT).astype(jnp.int32)


def scale_value(code):
    return jnp.exp2(code.astype(jnp.float32) * (1.0 / SCALE_UNIT))


def nearest(x):
    return jnp.floor(x + 0.5).astype(jnp.int32)


def peer(me, code):
    x = lax.rem(me // 8 + code // 8, 4)
    y = lax.rem((me // 2) % 4 + (code // 2) % 4, 4)
    z = lax.rem(me % 2 + code % 2, 2)
    return x * 8 + y * 2 + z


def offset(me, source):
    x = lax.rem(me // 8 - source // 8 + 4, 4)
    y = lax.rem((me // 2) % 4 - (source // 2) % 4 + 4, 4)
    z = lax.rem(me % 2 - source % 2 + 2, 2)
    return x * 8 + y * 2 + z


def order(k):
    return lax.rem(k * 11, DP)


def kernel(
    master_ref, moment1_ref, moment2_ref, quant_ref, expo_ref, replica_ref, failed_ref, dest_ref,
    w_ref, m_ref, u_ref,
    master, moment1, moment2, quant, expo, replica, dest_v, failed_s, dest_s,
    part, parts, w_code, w_send, w_recv, w_rows, mv_code, mv_send, mv_recvs, mv_rows,
    scales, rows_s, slots_s, in_sem, part_ssem, part_rsem, w_ssem, w_rsem, mv_ssem, mv_rsem,
):
    me = lax.axis_index("dp")
    group = lax.axis_index("pipe")

    loads = [
        pltpu.make_async_copy(src, dst, in_sem.at[i])
        for i, (src, dst) in enumerate(
            (
                (quant_ref, quant),
                (expo_ref, expo),
                (dest_ref, dest_v),
                (dest_ref, dest_s),
                (failed_ref, failed_s),
                (master_ref, master),
                (moment1_ref, moment1),
                (replica_ref, replica),
                (moment2_ref, moment2),
            )
        )
    ]
    barrier = pltpu.get_barrier_semaphore()

    def greet(c, carry):
        pl.semaphore_signal(
            barrier,
            inc=1,
            device_id=(lax.rem(me + c // PIPE, DP), lax.rem(group + c % PIPE, PIPE)),
            device_id_type=MESH,
        )
        return carry

    loads[0].start()
    loads[1].start()
    lax.fori_loop(1, DP * PIPE, greet, 0)
    for load in loads[2:]:
        load.start()

    loads[0].wait()
    loads[1].wait()
    line = lax.broadcasted_iota(jnp.int32, (K, K), 0)
    place = lax.broadcasted_iota(jnp.int32, (K, K), 1)
    expo_rows = jnp.sum(
        jnp.where(line == place, jnp.broadcast_to(expo[...].astype(jnp.float32), (K, K)), 0.0),
        axis=1,
        keepdims=True,
    )
    grad_scale = jnp.exp2(expo_rows)

    def scan_grad(step, carry):
        total, largest = carry
        x = quant[:, cols(step)].astype(jnp.float32)
        return total + x * x, jnp.maximum(largest, jnp.abs(x))

    zero_step = jnp.zeros((K, STEP_COLS), jnp.float32)
    total, largest = lax.fori_loop(0, D // STEP_COLS, scan_grad, (zero_step, zero_step))
    squares = fold(total, jnp.add) * (grad_scale * grad_scale)
    part[0:1, :] = jnp.sum(squares, axis=0, keepdims=True)
    grad_most = fold(largest, jnp.maximum) * ((1.0 - beta_one) * grad_scale)

    for load in loads[2:5]:
        load.wait()
    fail_a = failed_s[group, 0]
    fail_b = failed_s[group, 1]
    me_failed = (me == fail_a) | (me == fail_b)

    def find_slot(code, carry):
        target = peer(me, code)
        found = jnp.int32(0)
        for i in range(K):
            found = jnp.where((dest_s[group, me * K + i] >> 4) == target, i + 1, found)
        slots_s[code] = found
        return carry

    lax.fori_loop(0, DP, find_slot, 0)

    def row_for(code):
        found = slots_s[code]
        return jnp.maximum(found - 1, 0), found > 0

    dest_row = dest_v[pl.ds(group, 1), :]
    old_row = lax.broadcasted_iota(jnp.int32, (1, DP * K), 1)
    old_rank = old_row >> 4
    new_rank = dest_row >> 4
    rank_bit = lax.broadcasted_iota(jnp.int32, (1, DP), 1)
    alive_bits = jnp.sum(
        jnp.where((rank_bit == fail_a) | (rank_bit == fail_b), 0, 1 << rank_bit)
    )

    def helper_bits(receiver):
        bits = jnp.sum(jnp.where(new_rank == receiver, 1 << old_rank, 0))
        return alive_bits & ~bits

    def helper_row(receiver):
        bits = helper_bits(receiver)
        first = jnp.max(
            jnp.where((new_rank == receiver) & (old_rank == fail_a), old_row & 15, 0)
        )
        second = jnp.max(
            jnp.where((new_rank == receiver) & (old_rank == fail_b), old_row & 15, 0)
        )
        able = ((bits >> me) & 1) == 1
        lower = bits & ((1 << me) - 1)
        is_first = able & (lower == 0)
        is_second = able & (lower != 0) & ((lower & (lower - 1)) == 0)
        return jnp.where(is_first, K + first, jnp.where(is_second, 2 * K + second, 0))

    help_a = helper_row(fail_a)
    help_b = helper_row(fail_b)

    pl.semaphore_wait(barrier, DP * PIPE - 1)

    def part_copy(c):
        return pltpu.make_async_remote_copy(
            src_ref=part.at[pl.ds(0, 1)],
            dst_ref=parts.at[pl.ds(c, 1)],
            send_sem=part_ssem.at[c],
            recv_sem=part_rsem.at[c],
            device_id=(lax.rem(me + c // PIPE, DP), lax.rem(group + c % PIPE, PIPE)),
            device_id_type=MESH,
        )

    def send_part(c, carry):
        part_copy(c).start()
        return carry

    lax.fori_loop(1, DP * PIPE, send_part, 0)

    loads[5].wait()
    loads[6].wait()
    loads[7].wait()

    def weights(kind, step, base=0):
        if kind == 0:
            return master[:, cols(step, base=base)]
        rank = fail_a if kind == 1 else fail_b
        return replica[rank, :, cols(step, base=base)].astype(jnp.float32)

    def scan_moment(step, largest):
        return jnp.maximum(largest, jnp.abs(moment1[:, cols(step)]))

    keep = jnp.where(me_failed, 0.0, 1.0).astype(jnp.float32)
    largest = lax.fori_loop(0, D // STEP_COLS, scan_moment, zero_step)
    moment_code = scale_code(fold(largest, jnp.maximum) * (keep * beta_one))
    grad_code = scale_code(grad_most)
    scales[0:K, :] = scale_value(moment_code)
    scales[K : 2 * K, :] = scale_value(grad_code)

    for kind in range(3):
        rows = pl.ds(kind * K, K)

        def scan_weights(step, largest, kind=kind):
            return jnp.maximum(largest, jnp.abs(weights(kind, step)))

        largest = lax.fori_loop(0, D // STEP_COLS, scan_weights, zero_step)
        code = scale_code(fold(largest, jnp.maximum))
        to_code = tiled(32767.0 / scale_value(code))
        w_code[rows, HALF : HALF + LANES] = code
        w_code[rows, HALF + LANES : HALF + 2 * LANES] = moment_code
        w_code[rows, HALF + 2 * LANES : HALF + 3 * LANES] = grad_code

        def code_weights(step, carry, kind=kind, rows=rows, to_code=to_code):
            low = nearest(weights(kind, step) * to_code)
            high = nearest(weights(kind, step, HALF) * to_code)
            w_code[rows, cols(step)] = (high << 16) | (low & 0xFFFF)
            return carry

        lax.fori_loop(0, HALF // STEP_COLS, code_weights, 0)

    def w_copy(k):
        code = order(k)
        return pltpu.make_async_remote_copy(
            src_ref=w_send.at[pl.ds(code, 1)],
            dst_ref=w_recv.at[pl.ds(code, 1)],
            send_sem=w_ssem.at[code],
            recv_sem=w_rsem.at[code],
            device_id=(peer(me, code), group),
            device_id_type=MESH,
        )

    def w_slot(k):
        code = order(k)
        target = peer(me, code)
        row, has = row_for(code)
        helped = jnp.where(target == fail_a, help_a, jnp.where(target == fail_b, help_b, 0))
        w_send[pl.ds(code, 1), :] = w_code[pl.ds(jnp.where(has, row, helped), 1), :]

    def send_w(k, carry):
        w_slot(k)
        w_copy(k - 1).start()
        return carry

    w_slot(1)
    lax.fori_loop(2, DP, send_w, 0)
    w_copy(DP - 1).start()
    own_row, _ = row_for(0)
    w_recv[0:1, :] = w_code[pl.ds(own_row, 1), :]

    def find_row(j, taken):
        row = jnp.max(jnp.where(dest_row == me * K + j, old_row, 0))
        rows_s[j] = row
        return taken

    lax.fori_loop(0, K, find_row, 0)
    bits = helper_bits(me)
    lane = lax.broadcasted_iota(jnp.int32, (1, LANES), 1)
    able = (lane < DP) & (((bits >> (lane & 31)) & 1) == 1)
    helper_one = jnp.min(jnp.where(able, lane, DP - 1))
    helper_two = jnp.min(jnp.where(able & (lane > helper_one), lane, DP - 1))

    def wait_part(c, carry):
        part_copy(c).wait_recv()
        return carry

    lax.fori_loop(1, DP * PIPE, wait_part, 0)
    loads[8].wait()
    parts[0:1, :] = part[0:1, :]
    grad_total = jnp.sum(
        jnp.sum(parts[...], axis=0, keepdims=True), axis=1, keepdims=True
    )
    clip = jnp.minimum(1.0, lax.rsqrt(grad_total / float(DP * PIPE * K * D) + clip_eps))

    bound = scales[0:K, :] + clip * scales[K : 2 * K, :]
    to_unit = tiled(1.0 / bound)
    clip_scale = grad_scale * clip

    def mv_copy(chunk, k):
        code = order(k)
        return pltpu.make_async_remote_copy(
            src_ref=mv_send.at[chunk, pl.ds(code, 1)],
            dst_ref=mv_recvs[chunk].at[pl.ds(code, 1)],
            send_sem=mv_ssem.at[chunk, code],
            recv_sem=mv_rsem.at[chunk, code],
            device_id=(peer(me, code), group),
            device_id_type=MESH,
        )

    def mv_slot(chunk, k):
        code = order(k)
        row, _ = row_for(code)
        mv_send[chunk, pl.ds(code, 1), :] = mv_code[chunk, pl.ds(row, 1), :]

    def send_chunk(chunk):
        def code_moments(step, carry):
            here = cols(chunk * (CW // STEP_COLS) + step)
            clipped = quant[:, here].astype(jnp.float32) * clip_scale
            first = (keep * beta_one) * moment1[:, here] + (1.0 - beta_one) * clipped
            second = (keep * beta_two) * moment2[:, here] + (1.0 - beta_two) * clipped * clipped
            root = jnp.sqrt(jnp.abs(first) * to_unit) * 32767.0
            high = nearest(jnp.where(first < 0.0, -root, root))
            level = (jnp.log2(jnp.maximum(second, 0.2)) - LOG_LOW) * LOG_UNIT
            low = nearest(jnp.clip(level, 0.0, 65535.0))
            mv_code[chunk, :, cols(step)] = (high << 16) | low
            return carry

        lax.fori_loop(0, CW // STEP_COLS, code_moments, 0)

        def send_mv(k, carry):
            mv_slot(chunk, k)
            mv_copy(chunk, k - 1).start()
            return carry

        mv_slot(chunk, 1)
        lax.fori_loop(2, DP, send_mv, 0)
        mv_copy(chunk, DP - 1).start()
        mv_recvs[chunk][0:1, :] = mv_code[chunk, pl.ds(own_row, 1), :]

    for chunk in range(CHUNKS):
        send_chunk(chunk)

    def wait_w(k, carry):
        w_copy(k).wait_recv()
        return carry

    lax.fori_loop(1, DP, wait_w, 0)

    def place_w(j, carry):
        row = rows_s[j]
        source = row >> 4
        in_second = source == fail_b
        lost = (source == fail_a) | in_second
        helper = jnp.where(in_second, helper_two, helper_one)
        sender = jnp.where(lost & me_failed, helper, source)
        from_peer = w_recv[pl.ds(offset(me, sender), 1), :]
        block = jnp.where(in_second, 2 * K, K)
        local = w_code[pl.ds(jnp.where(lost, block + (row & 15), 0), 1), :]
        lost_here = lost & jnp.logical_not(me_failed)
        w_rows[pl.ds(j, 1), 0:HALF + LANES] = jnp.where(
            lost_here, local[:, 0:HALF + LANES], from_peer[:, 0:HALF + LANES]
        )
        owner = w_recv[pl.ds(offset(me, source), 1), HALF + LANES : W_COLS]
        w_rows[pl.ds(j, 1), HALF + LANES : W_COLS] = owner
        parts[pl.ds(j, 1), :] = jnp.broadcast_to(jnp.where(lost, 1.0, 0.0), (1, LANES))
        return carry

    lax.fori_loop(0, K, place_w, 0)
    w_unit = tiled(scale_value(w_rows[:, HALF : HALF + LANES]) * (1.0 / 32767.0))

    def decode_w(step, carry):
        word = w_rows[:, cols(step)]
        w_ref[:, cols(step)] = ((word << 16) >> 16).astype(jnp.float32) * w_unit
        w_ref[:, cols(step, base=HALF)] = (word >> 16).astype(jnp.float32) * w_unit
        return carry

    lax.fori_loop(0, HALF // STEP_COLS, decode_w, 0)
    came_bound = scale_value(w_rows[:, HALF + LANES : HALF + 2 * LANES]) + clip * scale_value(
        w_rows[:, HALF + 2 * LANES : W_COLS]
    )
    from_unit = tiled(came_bound * (1.0 / (32767.0 * 32767.0)))
    row_lost = tiled(parts[0:K, :]) > 0.5

    def take_chunk(chunk):
        def wait_mv(k, carry):
            mv_copy(chunk, k).wait_recv()
            return carry

        lax.fori_loop(1, DP, wait_mv, 0)

        def place_mv(j, carry):
            source = rows_s[j] >> 4
            mv_rows[chunk, pl.ds(j, 1), :] = mv_recvs[chunk][
                pl.ds(offset(me, source), 1), :
            ]
            return carry

        lax.fori_loop(0, K, place_mv, 0)

        def decode_mv(step, carry):
            here = cols(chunk * (CW // STEP_COLS) + step)
            word = mv_rows[chunk, :, cols(step)]
            high = (word >> 16).astype(jnp.float32)
            low = (word & 0xFFFF).astype(jnp.float32)
            first = high * jnp.abs(high) * from_unit
            grown = jnp.exp2(low * (0.5 / LOG_UNIT) + 0.5 * (LOG_LOW - math.log2(corr_two)))
            m_ref[:, here] = first
            u_ref[:, here] = jnp.where(
                row_lost, jnp.abs(first) * math.sqrt(5.0 / corr_two), grown
            )
            return carry

        lax.fori_loop(0, CW // STEP_COLS, decode_mv, 0)

    for chunk in range(CHUNKS):
        take_chunk(chunk)

    def left_part(c, carry):
        part_copy(c).wait_send()
        return carry

    def left_w(k, carry):
        w_copy(k).wait_send()
        for chunk in range(CHUNKS):
            mv_copy(chunk, k).wait_send()
        return carry

    lax.fori_loop(1, DP * PIPE, left_part, 0)
    lax.fori_loop(1, DP, left_w, 0)


def local(master, moment1, moment2, quant_grad, grad_exponent, replica_params, failed, dest):
    f32, i32 = jnp.float32, jnp.int32
    hbm = pl.BlockSpec(memory_space=pl.ANY)
    vmem = pl.BlockSpec(memory_space=pltpu.VMEM)
    dma = pltpu.SemaphoreType.DMA
    start, first, root = pl.pallas_call(
        kernel,
        out_shape=(jax.ShapeDtypeStruct((K, D), f32),) * 3,
        in_specs=[hbm] * 8,
        out_specs=(vmem,) * 3,
        scratch_shapes=[
            pltpu.VMEM((K, D), f32),
            pltpu.VMEM((K, D), f32),
            pltpu.VMEM((K, D), f32),
            pltpu.VMEM((K, D), jnp.bfloat16),
            pltpu.VMEM((1, K), i32),
            pltpu.VMEM((DP, K, D), jnp.bfloat16),
            pltpu.VMEM((PIPE, DP * K), i32),
            pltpu.SMEM((PIPE, 2), i32),
            pltpu.SMEM((PIPE, DP * K), i32),
            pltpu.VMEM((8, LANES), f32),
            pltpu.VMEM((DP * PIPE, LANES), f32),
            pltpu.VMEM((3 * K, W_COLS), i32),
            pltpu.VMEM((DP, W_COLS), i32),
            pltpu.VMEM((DP, W_COLS), i32),
            pltpu.VMEM((K, W_COLS), i32),
            pltpu.VMEM((CHUNKS, K, CW), i32),
            pltpu.VMEM((CHUNKS, DP, CW), i32),
            [pltpu.VMEM((DP, CW), i32)] * CHUNKS,
            pltpu.VMEM((CHUNKS, K, CW), i32),
            pltpu.VMEM((2 * K, LANES), f32),
            pltpu.SMEM((K,), i32),
            pltpu.SMEM((DP,), i32),
            dma((9,)),
            dma((DP * PIPE,)),
            dma((DP * PIPE,)),
            dma((DP,)),
            dma((DP,)),
            dma((CHUNKS, DP)),
            dma((CHUNKS, DP)),
        ],
        compiler_params=pltpu.CompilerParams(
            collective_id=0, has_side_effects=True, vmem_limit_bytes=56 * 2**20
        ),
        name="recover_step",
    )(
        master[0],
        moment1[0],
        moment2[0],
        quant_grad[0],
        grad_exponent,
        replica_params[0, 0].reshape(DP, K, D),
        failed,
        dest,
    )
    direction = first / corr_one / (root + adam_eps) + decay_rate * start
    return (
        (start - learn_rate * direction)[None],
        first[None],
        (corr_two * root * root)[None],
    )


def solution(mesh):
    in_specs = (
        P("pipe", "dp", None),
        P("pipe", "dp", None),
        P("pipe", "dp", None),
        P("pipe", "dp", None),
        P("pipe", "dp"),
        P("pipe", "dp", None, None),
        P(),
        P(),
    )
    out_specs = (P("pipe", "dp", None), P("pipe", "dp", None), P("pipe", "dp", None))
    return jax.shard_map(local, mesh=mesh, in_specs=in_specs, out_specs=out_specs, check_vma=False)
```

```python
import functools
import math

import jax
import jax.numpy as jnp
from jax import lax
from jax.experimental import pallas as pl
from jax.experimental.pallas import tpu as pltpu
from jax.sharding import PartitionSpec as P

STEP = 20

beta_one = 0.9
beta_two = 0.95
learn_rate = 0.00015
decay_rate = 0.1
adam_eps = 1e-08
clip_eps = 1e-06

corr_one = 1.0 - beta_one**STEP
corr_two = 1.0 - beta_two**STEP

LOGICAL = pl.DeviceIdType.LOGICAL
DP = 32
PIPE = 4
K = 16
D = 8192
HALF = D // 2
LANES = 128
W_COLS = HALF + 3 * LANES
PIECES = (2048, 2048, 2048, 1024, 1024)
BASES = tuple(sum(PIECES[:i]) for i in range(len(PIECES)))
WIDE = 1024
TILES = WIDE // LANES
STRIDE = 5
EARLY = 8

SCALE_UNIT = 65536.0
TINY = 1e-30
LOG_LOW = -2.2
LOG_SPAN = 16.0
LOG_UNIT = 65535.0 / LOG_SPAN


def cols(step, base=0):
    return pl.ds(pl.multiple_of(base + step * WIDE, LANES), WIDE)


def tiled(scale):
    return jnp.concatenate([scale] * TILES, axis=1)


def fold(acc, op):
    out = acc[:, :LANES]
    for t in range(1, TILES):
        out = op(out, acc[:, t * LANES : (t + 1) * LANES])
    return out


def scale_code(scale):
    return jnp.ceil(jnp.log2(jnp.maximum(scale, TINY)) * SCALE_UNIT).astype(jnp.int32)


def scale_value(code):
    return jnp.exp2(code.astype(jnp.float32) * (1.0 / SCALE_UNIT))


def nearest(x):
    return jnp.floor(x + 0.5).astype(jnp.int32)


def kernel(
    master_ref, moment1_ref, moment2_ref, quant_ref, expo_ref, replica_ref, failed_ref, dest_ref,
    w_ref, r_ref, u_ref,
    master, moment1, moment2, quant, expo, replica, dest_v, failed_s, dest_s,
    part, near, parts, w_code, w_send, w_recv, w_rows, mv_code, mv_send, mv_recvs, mv_rows,
    scales, lost_rows, amount, w_slot_s, mv_slot_s, owner_s, sender_s, local_s,
    in_sem, near_sem, part_sem, w_sem, mv_sem,
):
    me = lax.axis_index("dp")
    group = lax.axis_index("pipe")

    def member(rank, section):
        return rank * PIPE + section

    def rank_at(c):
        return lax.rem(me + c, DP)

    loads = [
        pltpu.make_async_copy(src, dst, in_sem.at[i])
        for i, (src, dst) in enumerate(
            (
                (quant_ref, quant),
                (expo_ref, expo),
                (dest_ref, dest_v),
                (dest_ref, dest_s),
                (failed_ref, failed_s),
                (master_ref, master),
                (moment1_ref, moment1),
                (replica_ref, replica),
                (moment2_ref, moment2),
            )
        )
    ]
    barrier = pltpu.get_barrier_semaphore()

    def greet(device):
        pl.semaphore_signal(barrier, inc=1, device_id=device, device_id_type=LOGICAL)

    for q in range(1, PIPE):
        greet(member(me, lax.rem(group + q, PIPE)))
    for c in range(1, DP):
        greet(member(rank_at(c), group))
    for load in loads:
        load.start()

    loads[0].wait()
    loads[1].wait()
    line = lax.broadcasted_iota(jnp.int32, (K, K), 0)
    place = lax.broadcasted_iota(jnp.int32, (K, K), 1)
    expo_rows = jnp.sum(
        jnp.where(line == place, jnp.broadcast_to(expo[...].astype(jnp.float32), (K, K)), 0.0),
        axis=1,
        keepdims=True,
    )
    grad_scale = jnp.exp2(expo_rows)

    def scan_grad(step, carry):
        total, largest = carry
        x = quant[:, cols(step)].astype(jnp.float32)
        return total + x * x, jnp.maximum(largest, jnp.abs(x))

    zero_step = jnp.zeros((K, WIDE), jnp.float32)
    total, largest = lax.fori_loop(0, D // WIDE, scan_grad, (zero_step, zero_step))
    squares = fold(total, jnp.add) * (grad_scale * grad_scale)
    part[0:1, :] = jnp.sum(squares, axis=0, keepdims=True)
    grad_code = scale_code(fold(largest, jnp.maximum) * ((1.0 - beta_one) * grad_scale))

    for load in loads[2:5]:
        load.wait()
    fail_a = failed_s[0, group]
    fail_b = failed_s[1, group]
    me_failed = (me == fail_a) | (me == fail_b)

    held = jnp.int32(0)
    words = [jnp.int32(0)] * 4
    for i in range(K):
        target = dest_s[group, me * K + i] >> 4
        nibble = i << (4 * (target & 7))
        words = [word | jnp.where((target >> 3) == q, nibble, 0) for q, word in enumerate(words)]
        held = held | (1 << target)

    dest_row = dest_v[pl.ds(group, 1), :]
    old_row = lax.broadcasted_iota(jnp.int32, (1, DP * K), 1)
    old_rank = old_row >> 4
    new_rank = dest_row >> 4
    alive_bits = ~((1 << fail_a) | (1 << fail_b))

    def helper_bits(receiver):
        bits = jnp.sum(jnp.where(new_rank == receiver, 1 << old_rank, 0))
        return alive_bits & ~bits

    def helper_row(receiver):
        bits = helper_bits(receiver)
        first = jnp.max(jnp.where((new_rank == receiver) & (old_rank == fail_a), old_row & 15, 0))
        second = jnp.max(jnp.where((new_rank == receiver) & (old_rank == fail_b), old_row & 15, 0))
        able = ((bits >> me) & 1) == 1
        lower = bits & ((1 << me) - 1)
        is_first = able & (lower == 0)
        is_second = able & (lower != 0) & ((lower & (lower - 1)) == 0)
        return jnp.where(is_first, K + first, jnp.where(is_second, 2 * K + second, 0))

    help_a = helper_row(fail_a)
    help_b = helper_row(fail_b)

    def fill_slot(c, carry):
        target = rank_at(c)
        word = words[0]
        for q in range(1, 4):
            word = jnp.where((target >> 3) == q, words[q], word)
        row = (word >> (4 * (target & 7))) & 15
        helped = jnp.where(target == fail_a, help_a, jnp.where(target == fail_b, help_b, 0))
        mv_slot_s[c] = row
        w_slot_s[c] = jnp.where(((held >> target) & 1) == 1, row, helped)
        return carry

    lax.fori_loop(0, DP, fill_slot, 0)

    for load in loads[5:8]:
        load.wait()

    def weights(kind, step, base=0):
        if kind == 0:
            return master[:, cols(step, base)]
        rank = fail_a if kind == 1 else fail_b
        return replica[rank, :, cols(step, base)].astype(jnp.float32)

    def scan_moment(step, largest):
        return jnp.maximum(largest, jnp.abs(moment1[:, cols(step)]))

    keep = jnp.where(me_failed, 0.0, 1.0).astype(jnp.float32)
    largest = lax.fori_loop(0, D // WIDE, scan_moment, zero_step)
    moment_code = scale_code(fold(largest, jnp.maximum) * (keep * beta_one))
    scales[0:K, :] = scale_value(moment_code)
    scales[K : 2 * K, :] = scale_value(grad_code)

    for kind in range(3):
        rows = pl.ds(kind * K, K)

        def scan_weights(step, largest, kind=kind):
            return jnp.maximum(largest, jnp.abs(weights(kind, step)))

        largest = lax.fori_loop(0, D // WIDE, scan_weights, zero_step)
        code = scale_code(fold(largest, jnp.maximum))
        to_code = tiled(32767.0 / scale_value(code))
        w_code[rows, HALF : HALF + LANES] = code
        w_code[rows, HALF + LANES : HALF + 2 * LANES] = moment_code
        w_code[rows, HALF + 2 * LANES : HALF + 3 * LANES] = grad_code

        def code_weights(step, carry, kind=kind, rows=rows, to_code=to_code):
            low = nearest(weights(kind, step) * to_code)
            high = nearest(weights(kind, step, HALF) * to_code)
            w_code[rows, cols(step)] = (high << 16) | (low & 0xFFFF)
            return carry

        lax.fori_loop(0, HALF // WIDE, code_weights, 0)

    pl.semaphore_wait(barrier, PIPE - 1 + DP - 1)

    def waiting(slots, width, sem):
        held_bytes = amount.at[pl.ds(0, slots), :, pl.ds(0, width)]
        return pltpu.make_async_copy(held_bytes, held_bytes, sem)

    def send(src, dst, sems, device):
        pltpu.make_async_remote_copy(
            src_ref=src,
            dst_ref=dst,
            send_sem=sems.at[0],
            recv_sem=sems.at[1],
            device_id=device,
            device_id_type=LOGICAL,
        ).start()

    for q in range(1, PIPE):
        send(
            part.at[pl.ds(0, 1)],
            near.at[pl.ds(q - 1, 1)],
            near_sem,
            member(me, lax.rem(group + q, PIPE)),
        )

    def slot_of(k):
        return lax.rem(k * STRIDE, DP)

    def fill_w(k):
        c = slot_of(k)
        w_send[pl.ds(c - 1, 1), :] = w_code[pl.ds(w_slot_s[c], 1), :]

    def send_w(k):
        c = slot_of(k)
        send(
            w_send.at[pl.ds(c - 1, 1)],
            w_recv.at[pl.ds(c - 1, 1)],
            w_sem,
            member(rank_at(c), group),
        )

    def step_w(k, carry):
        fill_w(k)
        send_w(k - 1)
        return carry

    fill_w(1)
    lax.fori_loop(2, EARLY + 2, step_w, 0)

    waiting(PIPE - 1, LANES, near_sem.at[1]).wait()
    own_part = part[0:1, :] + near[0:1, :] + near[1:2, :] + near[2:3, :]
    parts[DP - 1 : DP, :] = own_part
    for k in range(1, DP):
        c = (k * STRIDE) % DP
        send(
            parts.at[pl.ds(DP - 1, 1)],
            parts.at[pl.ds(c - 1, 1)],
            part_sem,
            member(rank_at(c), group),
        )
    lax.fori_loop(EARLY + 2, DP, step_w, 0)
    send_w(DP - 1)
    w_recv[DP - 1 : DP, :] = w_code[pl.ds(w_slot_s[0], 1), :]

    bits = helper_bits(me)
    lane = lax.broadcasted_iota(jnp.int32, (1, LANES), 1)
    able = (lane < DP) & (((bits >> (lane & 31)) & 1) == 1)
    helper_one = jnp.min(jnp.where(able, lane, DP - 1))
    helper_two = jnp.min(jnp.where(able & (lane > helper_one), lane, DP - 1))

    def slot_from(rank):
        return (me - rank + (DP - 1)) & (DP - 1)

    def find_row(j, carry):
        row = jnp.max(jnp.where(dest_row == me * K + j, old_row, 0))
        owner = row >> 4
        in_second = owner == fail_b
        lost = (owner == fail_a) | in_second
        helper = jnp.where(in_second, helper_two, helper_one)
        block = jnp.where(in_second, 2 * K, K)
        owner_s[j] = slot_from(owner)
        sender_s[j] = slot_from(jnp.where(lost & me_failed, helper, owner))
        local_s[j] = jnp.where(lost & jnp.logical_not(me_failed), block + (row & 15), 0)
        lost_rows[pl.ds(j, 1), :] = jnp.broadcast_to(jnp.where(lost, 1.0, 0.0), (1, LANES))
        return carry

    lax.fori_loop(0, K, find_row, 0)

    loads[8].wait()
    waiting(DP - 1, LANES, part_sem.at[1]).wait()
    grad_total = jnp.sum(jnp.sum(parts[...], axis=0, keepdims=True), axis=1, keepdims=True)
    clip = jnp.minimum(1.0, lax.rsqrt(grad_total / float(DP * PIPE * K * D) + clip_eps))

    bound = scales[0:K, :] + clip * scales[K : 2 * K, :]
    to_unit = tiled(1.0 / bound)
    clip_scale = grad_scale * clip

    def code_moments(step, carry):
        here = cols(step)
        clipped = quant[:, here].astype(jnp.float32) * clip_scale
        first = (keep * beta_one) * moment1[:, here] + (1.0 - beta_one) * clipped
        second = (keep * beta_two) * moment2[:, here] + (1.0 - beta_two) * clipped * clipped
        root = jnp.sqrt(jnp.abs(first) * to_unit) * 32767.0
        high = nearest(jnp.where(first < 0.0, -root, root))
        level = (jnp.log2(jnp.maximum(second, 0.2)) - LOG_LOW) * LOG_UNIT
        low = nearest(jnp.clip(level, 0.0, 65535.0))
        mv_code[:, here] = (high << 16) | low
        return carry

    for piece, (base, width) in enumerate(zip(BASES, PIECES)):
        lax.fori_loop(base // WIDE, (base + width) // WIDE, code_moments, 0)
        span = pl.ds(base, width)

        def fill_mv(k, span=span):
            c = slot_of(k)
            mv_send[pl.ds(c - 1, 1), span] = mv_code[pl.ds(mv_slot_s[c], 1), span]

        def send_mv(k, span=span, piece=piece):
            c = slot_of(k)
            send(
                mv_send.at[pl.ds(c - 1, 1), span],
                mv_recvs[piece].at[pl.ds(c - 1, 1)],
                mv_sem.at[piece],
                member(rank_at(c), group),
            )

        def step_mv(k, carry, fill=fill_mv, send_one=send_mv):
            fill(k)
            send_one(k - 1)
            return carry

        fill_mv(1)
        lax.fori_loop(2, DP, step_mv, 0)
        send_mv(DP - 1)
        mv_recvs[piece][DP - 1 : DP, :] = mv_code[pl.ds(mv_slot_s[0], 1), span]

    waiting(DP - 1, W_COLS, w_sem.at[1]).wait()

    def place_w(j, carry):
        local = local_s[j]
        from_peer = w_recv[pl.ds(sender_s[j], 1), 0 : HALF + LANES]
        from_here = w_code[pl.ds(local, 1), 0 : HALF + LANES]
        w_rows[pl.ds(j, 1), 0 : HALF + LANES] = jnp.where(local > 0, from_here, from_peer)
        w_rows[pl.ds(j, 1), HALF + LANES : W_COLS] = w_recv[
            pl.ds(owner_s[j], 1), HALF + LANES : W_COLS
        ]
        return carry

    lax.fori_loop(0, K, place_w, 0)
    w_unit = tiled(scale_value(w_rows[:, HALF : HALF + LANES]) * (1.0 / 32767.0))

    def decode_w(step, carry):
        word = w_rows[:, cols(step)]
        w_ref[:, cols(step)] = ((word << 16) >> 16).astype(jnp.float32) * w_unit
        w_ref[:, cols(step, HALF)] = (word >> 16).astype(jnp.float32) * w_unit
        return carry

    lax.fori_loop(0, HALF // WIDE, decode_w, 0)
    came_bound = scale_value(w_rows[:, HALF + LANES : HALF + 2 * LANES]) + clip * scale_value(
        w_rows[:, HALF + 2 * LANES : W_COLS]
    )
    from_unit = tiled(jnp.sqrt(came_bound) * (1.0 / 32767.0))
    row_lost = tiled(lost_rows[...]) > 0.5

    def decode_mv(step, carry):
        here = cols(step)
        word = mv_rows[:, here]
        signed_root = (word >> 16).astype(jnp.float32) * from_unit
        low = (word & 0xFFFF).astype(jnp.float32)
        grown = jnp.exp2(low * (0.5 / LOG_UNIT) + 0.5 * (LOG_LOW - math.log2(corr_two)))
        r_ref[:, here] = signed_root
        u_ref[:, here] = jnp.where(
            row_lost, signed_root * signed_root * math.sqrt(5.0 / corr_two), grown
        )
        return carry

    for piece, (base, width) in enumerate(zip(BASES, PIECES)):
        waiting(DP - 1, width, mv_sem.at[piece, 1]).wait()

        def place_mv(j, carry, piece=piece, base=base, width=width):
            mv_rows[pl.ds(j, 1), pl.ds(base, width)] = mv_recvs[piece][pl.ds(owner_s[j], 1), :]
            return carry

        lax.fori_loop(0, K, place_mv, 0)
        lax.fori_loop(base // WIDE, (base + width) // WIDE, decode_mv, 0)

    waiting(PIPE - 1, LANES, near_sem.at[0]).wait()
    waiting(DP - 1, LANES, part_sem.at[0]).wait()
    waiting(DP - 1, W_COLS, w_sem.at[0]).wait()
    for piece, width in enumerate(PIECES):
        waiting(DP - 1, width, mv_sem.at[piece, 0]).wait()


def local(master, moment1, moment2, quant_grad, grad_exponent, replica_params, failed, dest):
    f32, i32 = jnp.float32, jnp.int32
    hbm = pl.BlockSpec(memory_space=pltpu.HBM)
    vmem = pl.BlockSpec(memory_space=pltpu.VMEM)
    dma = pltpu.SemaphoreType.DMA
    start, signed_root, root = pl.pallas_call(
        kernel,
        out_shape=(jax.ShapeDtypeStruct((K, D), f32),) * 3,
        in_specs=[hbm] * 8,
        out_specs=(vmem,) * 3,
        scratch_shapes=[
            pltpu.VMEM((K, D), f32),
            pltpu.VMEM((K, D), f32),
            pltpu.VMEM((K, D), f32),
            pltpu.VMEM((K, D), jnp.bfloat16),
            pltpu.VMEM((1, K), i32),
            pltpu.VMEM((DP, K, D), jnp.bfloat16),
            pltpu.VMEM((PIPE, DP * K), i32),
            pltpu.SMEM((2, PIPE), i32),
            pltpu.SMEM((PIPE, DP * K), i32),
            pltpu.VMEM((8, LANES), f32),
            pltpu.VMEM((8, LANES), f32),
            pltpu.VMEM((DP, LANES), f32),
            pltpu.VMEM((3 * K, W_COLS), i32),
            pltpu.VMEM((DP, W_COLS), i32),
            pltpu.VMEM((DP, W_COLS), i32),
            pltpu.VMEM((K, W_COLS), i32),
            pltpu.VMEM((K, D), i32),
            pltpu.VMEM((DP, D), i32),
            [pltpu.VMEM((DP, width), i32) for width in PIECES],
            pltpu.VMEM((K, D), i32),
            pltpu.VMEM((2 * K, LANES), f32),
            pltpu.VMEM((K, LANES), f32),
            pltpu.VMEM((DP - 1, 1, W_COLS), i32),
            pltpu.SMEM((DP,), i32),
            pltpu.SMEM((DP,), i32),
            pltpu.SMEM((K,), i32),
            pltpu.SMEM((K,), i32),
            pltpu.SMEM((K,), i32),
            dma((9,)),
            dma((2,)),
            dma((2,)),
            dma((2,)),
            dma((len(PIECES), 2)),
        ],
        compiler_params=pltpu.CompilerParams(
            collective_id=0, has_side_effects=True, vmem_limit_bytes=24 * 2**20
        ),
        name="recover_step",
    )(
        *(
            pltpu.with_memory_space_constraint(x, pltpu.HBM)
            for x in (
                master[0],
                moment1[0],
                moment2[0],
                quant_grad[0],
                grad_exponent,
                replica_params[0, 0].reshape(DP, K, D),
                failed.T,
                dest,
            )
        )
    )
    first = signed_root * jnp.abs(signed_root)
    direction = first / corr_one / (root + adam_eps) + decay_rate * start
    return (
        (start - learn_rate * direction)[None],
        first[None],
        (corr_two * root * root)[None],
    )


def solution(mesh):
    in_specs = (
        P("pipe", "dp", None),
        P("pipe", "dp", None),
        P("pipe", "dp", None),
        P("pipe", "dp", None),
        P("pipe", "dp"),
        P("pipe", "dp", None, None),
        P(),
        P(),
    )
    out_specs = (P("pipe", "dp", None), P("pipe", "dp", None), P("pipe", "dp", None))
    return jax.shard_map(local, mesh=mesh, in_specs=in_specs, out_specs=out_specs, check_vma=False)
```

```python
import functools
import math

import jax
import jax.numpy as jnp
from jax import lax
from jax.experimental import pallas as pl
from jax.experimental.pallas import tpu as pltpu
from jax.sharding import PartitionSpec as P

STEP = 20

beta_one = 0.9
beta_two = 0.95
learn_rate = 0.00015
decay_rate = 0.1
adam_eps = 1e-08
clip_eps = 1e-06

corr_one = 1.0 - beta_one**STEP
corr_two = 1.0 - beta_two**STEP

LOGICAL = pl.DeviceIdType.LOGICAL
DP = 32
PIPE = 4
K = 16
D = 8192
HALF = D // 2
LANES = 128
W_COLS = HALF + 3 * LANES
PIECES = (2048, 2048, 2048, 1024, 1024)
BASES = tuple(sum(PIECES[:i]) for i in range(len(PIECES)))
WIDE = 1024
TILES = WIDE // LANES
STRIDE = 5
EARLY = 8

SCALE_UNIT = 65536.0
TINY = 1e-30
LOG_LOW = -2.2
LOG_SPAN = 16.0
LOG_UNIT = 65535.0 / LOG_SPAN


def cols(step, base=0):
    return pl.ds(pl.multiple_of(base + step * WIDE, LANES), WIDE)


def tiled(scale):
    return jnp.concatenate([scale] * TILES, axis=1)


def fold(acc, op):
    out = acc[:, :LANES]
    for t in range(1, TILES):
        out = op(out, acc[:, t * LANES : (t + 1) * LANES])
    return out


def scale_code(scale):
    return jnp.ceil(jnp.log2(jnp.maximum(scale, TINY)) * SCALE_UNIT).astype(jnp.int32)


def scale_value(code):
    return jnp.exp2(code.astype(jnp.float32) * (1.0 / SCALE_UNIT))


def nearest(x):
    return jnp.floor(x + 0.5).astype(jnp.int32)


def kernel(
    master_ref, moment1_ref, moment2_ref, quant_ref, expo_ref, replica_ref, failed_ref, dest_ref,
    w_ref, r_ref, u_ref,
    master, moment1, moment2, quant, expo, replica, dest_v, failed_s, dest_s,
    part, near_parts, y_parts, x_parts, w_code, w_send, w_recv, w_rows, mv_code, mv_send, mv_recvs, mv_rows,
    scales, lost_rows, amount, w_slot_s, mv_slot_s, owner_s, sender_s, local_s,
    y_in, x_in, in_sem, near_sem, y_sem, x_sem, w_sem, mv_sem,
):
    me = lax.axis_index("dp")
    group = lax.axis_index("pipe")

    def member(rank, section):
        return rank * PIPE + section

    def rank_at(c):
        return lax.rem(me + c, DP)

    loads = [
        pltpu.make_async_copy(src, dst, in_sem.at[i])
        for i, (src, dst) in enumerate(
            (
                (quant_ref, quant),
                (expo_ref, expo),
                (dest_ref, dest_v),
                (dest_ref, dest_s),
                (failed_ref, failed_s),
                (master_ref, master),
                (moment1_ref, moment1),
                (replica_ref, replica),
                (moment2_ref, moment2),
            )
        )
    ]
    barrier = pltpu.get_barrier_semaphore()

    def greet(device):
        pl.semaphore_signal(barrier, inc=1, device_id=device, device_id_type=LOGICAL)

    flat = member(me, group)
    column = [flat // 8 * 8 + lax.rem(flat + q, 8) for q in range(1, 8)]
    along_y = [flat // 32 * 32 + lax.rem(flat + 8 * q, 32) for q in range(1, 4)]
    along_x = [lax.rem(flat + 32 * q, 128) for q in range(1, 4)]
    for device in (*column, *along_y, *along_x):
        greet(device)
    for load in loads:
        load.start()

    loads[0].wait()
    loads[1].wait()
    line = lax.broadcasted_iota(jnp.int32, (K, K), 0)
    place = lax.broadcasted_iota(jnp.int32, (K, K), 1)
    expo_rows = jnp.sum(
        jnp.where(line == place, jnp.broadcast_to(expo[...].astype(jnp.float32), (K, K)), 0.0),
        axis=1,
        keepdims=True,
    )
    grad_scale = jnp.exp2(expo_rows)

    def scan_grad(step, carry):
        total, largest = carry
        x = quant[:, cols(step)].astype(jnp.float32)
        return total + x * x, jnp.maximum(largest, jnp.abs(x))

    zero_step = jnp.zeros((K, WIDE), jnp.float32)
    total, largest = lax.fori_loop(0, D // WIDE, scan_grad, (zero_step, zero_step))
    squares = fold(total, jnp.add) * (grad_scale * grad_scale)
    part[0:1, :] = jnp.sum(squares, axis=0, keepdims=True)
    grad_code = scale_code(fold(largest, jnp.maximum) * ((1.0 - beta_one) * grad_scale))

    def waiting(slots, width, sem):
        held_bytes = amount.at[pl.ds(0, slots), :, pl.ds(0, width)]
        return pltpu.make_async_copy(held_bytes, held_bytes, sem)

    def send(src, dst, sems, device):
        pltpu.make_async_remote_copy(
            src_ref=src,
            dst_ref=dst,
            send_sem=sems.at[0],
            recv_sem=sems.at[1],
            device_id=device,
            device_id_type=LOGICAL,
        ).start()

    pl.semaphore_wait(barrier, 13)
    for q, device in enumerate(column):
        send(part.at[pl.ds(0, 1)], near_parts.at[pl.ds(q, 1)], near_sem, device)
    for device in along_y:
        pl.semaphore_signal(y_in, inc=1, device_id=device, device_id_type=LOGICAL)

    for load in loads[2:5]:
        load.wait()
    fail_a = failed_s[0, group]
    fail_b = failed_s[1, group]
    me_failed = (me == fail_a) | (me == fail_b)

    held = jnp.int32(0)
    words = [jnp.int32(0)] * 4
    for i in range(K):
        target = dest_s[group, me * K + i] >> 4
        nibble = i << (4 * (target & 7))
        words = [word | jnp.where((target >> 3) == q, nibble, 0) for q, word in enumerate(words)]
        held = held | (1 << target)

    dest_row = dest_v[pl.ds(group, 1), :]
    old_row = lax.broadcasted_iota(jnp.int32, (1, DP * K), 1)
    old_rank = old_row >> 4
    new_rank = dest_row >> 4
    alive_bits = ~((1 << fail_a) | (1 << fail_b))

    def helper_bits(receiver):
        bits = jnp.sum(jnp.where(new_rank == receiver, 1 << old_rank, 0))
        return alive_bits & ~bits

    def helper_row(receiver):
        bits = helper_bits(receiver)
        first = jnp.max(jnp.where((new_rank == receiver) & (old_rank == fail_a), old_row & 15, 0))
        second = jnp.max(jnp.where((new_rank == receiver) & (old_rank == fail_b), old_row & 15, 0))
        able = ((bits >> me) & 1) == 1
        lower = bits & ((1 << me) - 1)
        is_first = able & (lower == 0)
        is_second = able & (lower != 0) & ((lower & (lower - 1)) == 0)
        return jnp.where(is_first, K + first, jnp.where(is_second, 2 * K + second, 0))

    help_a = helper_row(fail_a)
    help_b = helper_row(fail_b)

    def fill_slot(c, carry):
        target = rank_at(c)
        word = words[0]
        for q in range(1, 4):
            word = jnp.where((target >> 3) == q, words[q], word)
        row = (word >> (4 * (target & 7))) & 15
        helped = jnp.where(target == fail_a, help_a, jnp.where(target == fail_b, help_b, 0))
        mv_slot_s[c] = row
        w_slot_s[c] = jnp.where(((held >> target) & 1) == 1, row, helped)
        return carry

    lax.fori_loop(0, DP, fill_slot, 0)

    for load in loads[5:8]:
        load.wait()

    def weights(kind, step, base=0):
        if kind == 0:
            return master[:, cols(step, base)]
        rank = fail_a if kind == 1 else fail_b
        return replica[rank, :, cols(step, base)].astype(jnp.float32)

    def scan_moment(step, largest):
        return jnp.maximum(largest, jnp.abs(moment1[:, cols(step)]))

    keep = jnp.where(me_failed, 0.0, 1.0).astype(jnp.float32)
    largest = lax.fori_loop(0, D // WIDE, scan_moment, zero_step)
    moment_code = scale_code(fold(largest, jnp.maximum) * (keep * beta_one))
    scales[0:K, :] = scale_value(moment_code)
    scales[K : 2 * K, :] = scale_value(grad_code)

    for kind in range(3):
        rows = pl.ds(kind * K, K)

        def scan_weights(step, largest, kind=kind):
            return jnp.maximum(largest, jnp.abs(weights(kind, step)))

        largest = lax.fori_loop(0, D // WIDE, scan_weights, zero_step)
        code = scale_code(fold(largest, jnp.maximum))
        to_code = tiled(32767.0 / scale_value(code))
        w_code[rows, HALF : HALF + LANES] = code
        w_code[rows, HALF + LANES : HALF + 2 * LANES] = moment_code
        w_code[rows, HALF + 2 * LANES : HALF + 3 * LANES] = grad_code

        def code_weights(step, carry, kind=kind, rows=rows, to_code=to_code):
            low = nearest(weights(kind, step) * to_code)
            high = nearest(weights(kind, step, HALF) * to_code)
            w_code[rows, cols(step)] = (high << 16) | (low & 0xFFFF)
            return carry

        lax.fori_loop(0, HALF // WIDE, code_weights, 0)

    pl.semaphore_wait(y_in, 3)
    for device in along_x:
        pl.semaphore_signal(x_in, inc=1, device_id=device, device_id_type=LOGICAL)

    waiting(7, LANES, near_sem.at[1]).wait()
    part[1:2, :] = part[0:1, :] + jnp.sum(near_parts[0:7, :], axis=0, keepdims=True)
    for q, device in enumerate(along_y):
        send(part.at[pl.ds(1, 1)], y_parts.at[pl.ds(q, 1)], y_sem, device)

    pl.semaphore_wait(x_in, 3)

    def slot_of(k):
        return lax.rem(k * STRIDE, DP)

    def fill_w(k):
        c = slot_of(k)
        w_send[pl.ds(c - 1, 1), :] = w_code[pl.ds(w_slot_s[c], 1), :]

    def send_w(k):
        c = slot_of(k)
        send(
            w_send.at[pl.ds(c - 1, 1)],
            w_recv.at[pl.ds(c - 1, 1)],
            w_sem,
            member(rank_at(c), group),
        )

    def step_w(k, carry):
        fill_w(k)
        send_w(k - 1)
        return carry

    fill_w(1)
    lax.fori_loop(2, EARLY + 2, step_w, 0)

    waiting(3, LANES, y_sem.at[1]).wait()
    part[2:3, :] = part[1:2, :] + jnp.sum(y_parts[0:3, :], axis=0, keepdims=True)
    for q, device in enumerate(along_x):
        send(part.at[pl.ds(2, 1)], x_parts.at[pl.ds(q, 1)], x_sem, device)
    lax.fori_loop(EARLY + 2, DP, step_w, 0)
    send_w(DP - 1)
    w_recv[DP - 1 : DP, :] = w_code[pl.ds(w_slot_s[0], 1), :]

    bits = helper_bits(me)
    lane = lax.broadcasted_iota(jnp.int32, (1, LANES), 1)
    able = (lane < DP) & (((bits >> (lane & 31)) & 1) == 1)
    helper_one = jnp.min(jnp.where(able, lane, DP - 1))
    helper_two = jnp.min(jnp.where(able & (lane > helper_one), lane, DP - 1))

    def slot_from(rank):
        return (me - rank + (DP - 1)) & (DP - 1)

    def find_row(j, carry):
        row = jnp.max(jnp.where(dest_row == me * K + j, old_row, 0))
        owner = row >> 4
        in_second = owner == fail_b
        lost = (owner == fail_a) | in_second
        helper = jnp.where(in_second, helper_two, helper_one)
        block = jnp.where(in_second, 2 * K, K)
        owner_s[j] = slot_from(owner)
        sender_s[j] = slot_from(jnp.where(lost & me_failed, helper, owner))
        local_s[j] = jnp.where(lost & jnp.logical_not(me_failed), block + (row & 15), 0)
        lost_rows[pl.ds(j, 1), :] = jnp.broadcast_to(jnp.where(lost, 1.0, 0.0), (1, LANES))
        return carry

    lax.fori_loop(0, K, find_row, 0)

    loads[8].wait()
    waiting(3, LANES, x_sem.at[1]).wait()
    grad_total = jnp.sum(
        part[2:3, :] + jnp.sum(x_parts[0:3, :], axis=0, keepdims=True), axis=1, keepdims=True
    )
    clip = jnp.minimum(1.0, lax.rsqrt(grad_total / float(DP * PIPE * K * D) + clip_eps))

    bound = scales[0:K, :] + clip * scales[K : 2 * K, :]
    to_unit = tiled(1.0 / bound)
    clip_scale = grad_scale * clip

    def code_moments(step, carry):
        here = cols(step)
        clipped = quant[:, here].astype(jnp.float32) * clip_scale
        first = (keep * beta_one) * moment1[:, here] + (1.0 - beta_one) * clipped
        second = (keep * beta_two) * moment2[:, here] + (1.0 - beta_two) * clipped * clipped
        root = jnp.sqrt(jnp.abs(first) * to_unit) * 32767.0
        high = nearest(jnp.where(first < 0.0, -root, root))
        level = (jnp.log2(jnp.maximum(second, 0.2)) - LOG_LOW) * LOG_UNIT
        low = nearest(jnp.clip(level, 0.0, 65535.0))
        mv_code[:, here] = (high << 16) | low
        return carry

    for piece, (base, width) in enumerate(zip(BASES, PIECES)):
        lax.fori_loop(base // WIDE, (base + width) // WIDE, code_moments, 0)
        span = pl.ds(base, width)

        def fill_mv(k, span=span):
            c = slot_of(k)
            mv_send[pl.ds(c - 1, 1), span] = mv_code[pl.ds(mv_slot_s[c], 1), span]

        def send_mv(k, span=span, piece=piece):
            c = slot_of(k)
            send(
                mv_send.at[pl.ds(c - 1, 1), span],
                mv_recvs[piece].at[pl.ds(c - 1, 1)],
                mv_sem.at[piece],
                member(rank_at(c), group),
            )

        def step_mv(k, carry, fill=fill_mv, send_one=send_mv):
            fill(k)
            send_one(k - 1)
            return carry

        fill_mv(1)
        lax.fori_loop(2, DP, step_mv, 0)
        send_mv(DP - 1)
        mv_recvs[piece][DP - 1 : DP, :] = mv_code[pl.ds(mv_slot_s[0], 1), span]

    waiting(DP - 1, W_COLS, w_sem.at[1]).wait()

    def place_w(j, carry):
        local = local_s[j]
        from_peer = w_recv[pl.ds(sender_s[j], 1), 0 : HALF + LANES]
        from_here = w_code[pl.ds(local, 1), 0 : HALF + LANES]
        w_rows[pl.ds(j, 1), 0 : HALF + LANES] = jnp.where(local > 0, from_here, from_peer)
        w_rows[pl.ds(j, 1), HALF + LANES : W_COLS] = w_recv[
            pl.ds(owner_s[j], 1), HALF + LANES : W_COLS
        ]
        return carry

    lax.fori_loop(0, K, place_w, 0)
    w_unit = tiled(scale_value(w_rows[:, HALF : HALF + LANES]) * (1.0 / 32767.0))

    def decode_w(step, carry):
        word = w_rows[:, cols(step)]
        w_ref[:, cols(step)] = ((word << 16) >> 16).astype(jnp.float32) * w_unit
        w_ref[:, cols(step, HALF)] = (word >> 16).astype(jnp.float32) * w_unit
        return carry

    lax.fori_loop(0, HALF // WIDE, decode_w, 0)
    came_bound = scale_value(w_rows[:, HALF + LANES : HALF + 2 * LANES]) + clip * scale_value(
        w_rows[:, HALF + 2 * LANES : W_COLS]
    )
    from_unit = tiled(jnp.sqrt(came_bound) * (1.0 / 32767.0))
    row_lost = tiled(lost_rows[...]) > 0.5

    def decode_mv(step, carry):
        here = cols(step)
        word = mv_rows[:, here]
        signed_root = (word >> 16).astype(jnp.float32) * from_unit
        low = (word & 0xFFFF).astype(jnp.float32)
        grown = jnp.exp2(low * (0.5 / LOG_UNIT) + 0.5 * (LOG_LOW - math.log2(corr_two)))
        r_ref[:, here] = signed_root
        u_ref[:, here] = jnp.where(
            row_lost, signed_root * signed_root * math.sqrt(5.0 / corr_two), grown
        )
        return carry

    for piece, (base, width) in enumerate(zip(BASES, PIECES)):
        waiting(DP - 1, width, mv_sem.at[piece, 1]).wait()

        def place_mv(j, carry, piece=piece, base=base, width=width):
            mv_rows[pl.ds(j, 1), pl.ds(base, width)] = mv_recvs[piece][pl.ds(owner_s[j], 1), :]
            return carry

        lax.fori_loop(0, K, place_mv, 0)
        lax.fori_loop(base // WIDE, (base + width) // WIDE, decode_mv, 0)

    waiting(7, LANES, near_sem.at[0]).wait()
    waiting(3, LANES, y_sem.at[0]).wait()
    waiting(3, LANES, x_sem.at[0]).wait()
    waiting(DP - 1, W_COLS, w_sem.at[0]).wait()
    for piece, width in enumerate(PIECES):
        waiting(DP - 1, width, mv_sem.at[piece, 0]).wait()


def local(master, moment1, moment2, quant_grad, grad_exponent, replica_params, failed, dest):
    f32, i32 = jnp.float32, jnp.int32
    hbm = pl.BlockSpec(memory_space=pltpu.HBM)
    vmem = pl.BlockSpec(memory_space=pltpu.VMEM)
    dma = pltpu.SemaphoreType.DMA
    start, signed_root, root = pl.pallas_call(
        kernel,
        out_shape=(jax.ShapeDtypeStruct((K, D), f32),) * 3,
        in_specs=[hbm] * 8,
        out_specs=(vmem,) * 3,
        scratch_shapes=[
            pltpu.VMEM((K, D), f32),
            pltpu.VMEM((K, D), f32),
            pltpu.VMEM((K, D), f32),
            pltpu.VMEM((K, D), jnp.bfloat16),
            pltpu.VMEM((1, K), i32),
            pltpu.VMEM((DP, K, D), jnp.bfloat16),
            pltpu.VMEM((PIPE, DP * K), i32),
            pltpu.SMEM((2, PIPE), i32),
            pltpu.SMEM((PIPE, DP * K), i32),
            pltpu.VMEM((8, LANES), f32),
            pltpu.VMEM((8, LANES), f32),
            pltpu.VMEM((8, LANES), f32),
            pltpu.VMEM((8, LANES), f32),
            pltpu.VMEM((3 * K, W_COLS), i32),
            pltpu.VMEM((DP, W_COLS), i32),
            pltpu.VMEM((DP, W_COLS), i32),
            pltpu.VMEM((K, W_COLS), i32),
            pltpu.VMEM((K, D), i32),
            pltpu.VMEM((DP, D), i32),
            [pltpu.VMEM((DP, width), i32) for width in PIECES],
            pltpu.VMEM((K, D), i32),
            pltpu.VMEM((2 * K, LANES), f32),
            pltpu.VMEM((K, LANES), f32),
            pltpu.VMEM((DP - 1, 1, W_COLS), i32),
            pltpu.SMEM((DP,), i32),
            pltpu.SMEM((DP,), i32),
            pltpu.SMEM((K,), i32),
            pltpu.SMEM((K,), i32),
            pltpu.SMEM((K,), i32),
            pltpu.SemaphoreType.REGULAR,
            pltpu.SemaphoreType.REGULAR,
            dma((9,)),
            dma((2,)),
            dma((2,)),
            dma((2,)),
            dma((2,)),
            dma((len(PIECES), 2)),
        ],
        compiler_params=pltpu.CompilerParams(
            collective_id=0, has_side_effects=True, vmem_limit_bytes=24 * 2**20
        ),
        name="recover_step",
    )(
        *(
            pltpu.with_memory_space_constraint(x, pltpu.HBM)
            for x in (
                master[0],
                moment1[0],
                moment2[0],
                quant_grad[0],
                grad_exponent,
                replica_params[0, 0].reshape(DP, K, D),
                failed.T,
                dest,
            )
        )
    )
    first = signed_root * jnp.abs(signed_root)
    direction = first / corr_one / (root + adam_eps) + decay_rate * start
    return (
        (start - learn_rate * direction)[None],
        first[None],
        (corr_two * root * root)[None],
    )


def solution(mesh):
    in_specs = (
        P("pipe", "dp", None),
        P("pipe", "dp", None),
        P("pipe", "dp", None),
        P("pipe", "dp", None),
        P("pipe", "dp"),
        P("pipe", "dp", None, None),
        P(),
        P(),
    )
    out_specs = (P("pipe", "dp", None), P("pipe", "dp", None), P("pipe", "dp", None))
    return jax.shard_map(local, mesh=mesh, in_specs=in_specs, out_specs=out_specs, check_vma=False)
```

```python
import functools
import math

import jax
import jax.numpy as jnp
from jax import lax
from jax.experimental import pallas as pl
from jax.experimental.pallas import tpu as pltpu
from jax.sharding import PartitionSpec as P

STEP = 20

beta_one = 0.9
beta_two = 0.95
learn_rate = 0.00015
decay_rate = 0.1
adam_eps = 1e-08
clip_eps = 1e-06

corr_one = 1.0 - beta_one**STEP
corr_two = 1.0 - beta_two**STEP

LOGICAL = pl.DeviceIdType.LOGICAL
DP = 32
PIPE = 4
K = 16
D = 8192
HALF = D // 2
LANES = 128
W_COLS = HALF + 3 * LANES
PIECES = (2048, 2048, 2048, 1024, 1024)
BASES = tuple(sum(PIECES[:i]) for i in range(len(PIECES)))
WIDE = 1024
TILES = WIDE // LANES
STRIDE = 5

SCALE_UNIT = 65536.0
TINY = 1e-30
LOG_LOW = -2.2
LOG_SPAN = 16.0
LOG_UNIT = 65535.0 / LOG_SPAN


def cols(step, base=0):
    return pl.ds(pl.multiple_of(base + step * WIDE, LANES), WIDE)


def tiled(scale):
    return jnp.concatenate([scale] * TILES, axis=1)


def fold(acc, op):
    out = acc[:, :LANES]
    for t in range(1, TILES):
        out = op(out, acc[:, t * LANES : (t + 1) * LANES])
    return out


def scale_code(scale):
    return jnp.ceil(jnp.log2(jnp.maximum(scale, TINY)) * SCALE_UNIT).astype(jnp.int32)


def scale_value(code):
    return jnp.exp2(code.astype(jnp.float32) * (1.0 / SCALE_UNIT))


def nearest(x):
    return jnp.floor(x + 0.5).astype(jnp.int32)


def kernel(
    master_ref, moment1_ref, moment2_ref, quant_ref, expo_ref, replica_ref, failed_ref, dest_ref,
    w_ref, r_ref, u_ref,
    master, moment1, moment2, quant, expo, replica, dest_v, failed_s, dest_s,
    part, near_parts, far_parts, w_code, w_send, w_recv, w_rows, mv_code, mv_send, mv_recvs, mv_rows,
    scales, lost_rows, amount, w_slot_s, mv_slot_s, owner_s, sender_s, local_s,
    y_in, x_in, in_sem, near_sem, far_sem, w_sem, mv_sem,
):
    me = lax.axis_index("dp")
    group = lax.axis_index("pipe")

    def member(rank, section):
        return rank * PIPE + section

    x0, y0, z0 = lax.div(me, 8), lax.rem(lax.div(me, 2), 4), lax.rem(me, 2)

    def rank_at(c):
        x = lax.rem(x0 + c // 8, 4)
        y = lax.rem(y0 + (c // 2) % 4, 4)
        return x * 8 + y * 2 + lax.rem(z0 + c % 2, 2)

    x_parts = [lax.rem(x0 + d, 4) * (8 * PIPE) for d in range(4)]
    y_parts = [lax.rem(y0 + d, 4) * (2 * PIPE) for d in range(4)]
    z_parts = [lax.rem(z0 + d, 2) * PIPE + group for d in range(2)]

    def device_at(c):
        return x_parts[c // 8] + y_parts[(c // 2) % 4] + z_parts[c % 2]

    loads = [
        pltpu.make_async_copy(src, dst, in_sem.at[i])
        for i, (src, dst) in enumerate(
            (
                (quant_ref, quant),
                (expo_ref, expo),
                (dest_ref, dest_v),
                (dest_ref, dest_s),
                (failed_ref, failed_s),
                (master_ref, master),
                (moment1_ref, moment1),
                (replica_ref, replica),
                (moment2_ref, moment2),
            )
        )
    ]
    barrier = pltpu.get_barrier_semaphore()

    def greet(device):
        pl.semaphore_signal(barrier, inc=1, device_id=device, device_id_type=LOGICAL)

    flat = member(me, group)
    column = [flat // 8 * 8 + lax.rem(flat + q, 8) for q in range(1, 8)]
    along_y = [flat // 32 * 32 + lax.rem(flat + 8 * q, 32) for q in range(1, 4)]
    along_x = [lax.rem(flat + 32 * q, 128) for q in range(1, 4)]
    for device in (*column, *along_y, *along_x):
        greet(device)
    for load in loads[:7]:
        load.start()

    loads[0].wait()
    loads[1].wait()
    line = lax.broadcasted_iota(jnp.int32, (K, K), 0)
    place = lax.broadcasted_iota(jnp.int32, (K, K), 1)
    expo_rows = jnp.sum(
        jnp.where(line == place, jnp.broadcast_to(expo[...].astype(jnp.float32), (K, K)), 0.0),
        axis=1,
        keepdims=True,
    )
    grad_scale = jnp.exp2(expo_rows)

    def scan_grad(step, carry):
        total, largest = carry
        x = quant[:, cols(step)].astype(jnp.float32)
        return total + x * x, jnp.maximum(largest, jnp.abs(x))

    zero_step = jnp.zeros((K, WIDE), jnp.float32)
    total, largest = lax.fori_loop(0, D // WIDE, scan_grad, (zero_step, zero_step))
    squares = fold(total, jnp.add) * (grad_scale * grad_scale)
    part[0:1, :] = jnp.sum(squares, axis=0, keepdims=True)
    grad_code = scale_code(fold(largest, jnp.maximum) * ((1.0 - beta_one) * grad_scale))

    def waiting(slots, width, sem):
        held_bytes = amount.at[pl.ds(0, slots), :, pl.ds(0, width)]
        return pltpu.make_async_copy(held_bytes, held_bytes, sem)

    def send(src, dst, sems, device):
        pltpu.make_async_remote_copy(
            src_ref=src,
            dst_ref=dst,
            send_sem=sems.at[0],
            recv_sem=sems.at[1],
            device_id=device,
            device_id_type=LOGICAL,
        ).start()

    pl.semaphore_wait(barrier, 13)
    for q, device in enumerate(column):
        send(part.at[pl.ds(0, 1)], near_parts.at[pl.ds(q, 1)], near_sem, device)
    for device in (*along_y, device_at(1)):
        pl.semaphore_signal(y_in, inc=1, device_id=device, device_id_type=LOGICAL)

    for load in loads[2:5]:
        load.wait()
    fail_a = failed_s[0, group]
    fail_b = failed_s[1, group]
    me_failed = (me == fail_a) | (me == fail_b)

    held = jnp.int32(0)
    words = [jnp.int32(0)] * 4
    for i in range(K):
        target = dest_s[group, me * K + i] >> 4
        nibble = i << (4 * (target & 7))
        words = [word | jnp.where((target >> 3) == q, nibble, 0) for q, word in enumerate(words)]
        held = held | (1 << target)

    dest_row = dest_v[pl.ds(group, 1), :]
    old_row = lax.broadcasted_iota(jnp.int32, (1, DP * K), 1)
    old_rank = old_row >> 4
    new_rank = dest_row >> 4
    alive_bits = ~((1 << fail_a) | (1 << fail_b))

    def fill_slot(c, carry):
        target = rank_at(c)
        word = words[0]
        for q in range(1, 4):
            word = jnp.where((target >> 3) == q, words[q], word)
        w_slot_s[c] = (word >> (4 * (target & 7))) & 15
        return carry

    lax.fori_loop(0, DP, fill_slot, 0)

    loads[5].wait()
    loads[6].wait()
    loads[7].start()
    loads[8].start()

    def scan_moment(step, largest):
        return jnp.maximum(largest, jnp.abs(moment1[:, cols(step)]))

    keep = jnp.where(me_failed, 0.0, 1.0).astype(jnp.float32)
    largest = lax.fori_loop(0, D // WIDE, scan_moment, zero_step)
    moment_code = scale_code(fold(largest, jnp.maximum) * (keep * beta_one))
    scales[0:K, :] = scale_value(moment_code)
    scales[K : 2 * K, :] = scale_value(grad_code)
    w_code[:, HALF + LANES : HALF + 2 * LANES] = moment_code
    w_code[:, HALF + 2 * LANES : HALF + 3 * LANES] = grad_code

    def code_block(weights, store):
        def scan_weights(step, largest):
            return jnp.maximum(largest, jnp.abs(weights(step)))

        largest = lax.fori_loop(0, D // WIDE, scan_weights, zero_step)
        code = scale_code(fold(largest, jnp.maximum))
        to_code = tiled(32767.0 / scale_value(code))
        store(pl.ds(HALF, LANES), code)

        def code_weights(step, carry):
            low = nearest(weights(step) * to_code)
            high = nearest(weights(step, HALF) * to_code)
            store(cols(step), (high << 16) | (low & 0xFFFF))
            return carry

        lax.fori_loop(0, HALF // WIDE, code_weights, 0)

    def store_own(span, value):
        w_code[:, span] = value

    code_block(lambda step, base=0: master[:, cols(step, base)], store_own)

    def fill_w(c):
        w_send[pl.ds(c - 1, 1), :] = w_code[pl.ds(w_slot_s[c], 1), :]

    def send_w(c):
        send(
            w_send.at[pl.ds(c - 1, 1)],
            w_recv.at[pl.ds(c - 1, 1)],
            w_sem,
            device_at(c),
        )

    for c in (1, 2, 8, 6, 24, 4, 16):
        fill_w(c)
    for c in (1, 2, 8, 6, 24, 4, 16):
        send_w(c)

    pl.semaphore_wait(y_in, 4)
    for device in along_x:
        pl.semaphore_signal(x_in, inc=1, device_id=device, device_id_type=LOGICAL)

    waiting(7, LANES, near_sem.at[1]).wait()
    part[1:2, :] = part[0:1, :] + jnp.sum(near_parts[0:7, :], axis=0, keepdims=True)
    for k in range(1, 16):
        q = (k * STRIDE) % 16
        send(
            part.at[pl.ds(1, 1)],
            far_parts.at[pl.ds(q - 1, 1)],
            far_sem,
            device_at(2 * q),
        )

    def send_group(codes):
        fill_w(codes[0])
        for before, c in zip(codes, codes[1:]):
            fill_w(c)
            send_w(before)
        send_w(codes[-1])

    send_group([3, 18, 9, 12, 5, 26, 17, 10, 7, 20, 25, 28, 14, 22, 30])
    pl.semaphore_wait(x_in, 3)
    send_group([21, 11, 31, 13, 27, 23, 19, 15, 29])
    w_recv[DP - 1 : DP, :] = w_code[pl.ds(w_slot_s[0], 1), :]

    def helper_bits(receiver):
        bits = jnp.sum(jnp.where(new_rank == receiver, 1 << old_rank, 0))
        return alive_bits & ~bits

    def helper_row(receiver):
        bits = helper_bits(receiver)
        first = jnp.max(jnp.where((new_rank == receiver) & (old_rank == fail_a), old_row & 15, 0))
        second = jnp.max(jnp.where((new_rank == receiver) & (old_rank == fail_b), old_row & 15, 0))
        able = ((bits >> me) & 1) == 1
        lower = bits & ((1 << me) - 1)
        is_first = able & (lower == 0)
        is_second = able & (lower != 0) & ((lower & (lower - 1)) == 0)
        return jnp.where(is_first, K + first, jnp.where(is_second, 2 * K + second, 0))

    help_a = helper_row(fail_a)
    help_b = helper_row(fail_b)

    help_a = helper_row(fail_a)
    help_b = helper_row(fail_b)

    def fill_help(c, carry):
        target = rank_at(c)
        helped = jnp.where(target == fail_a, help_a, jnp.where(target == fail_b, help_b, 0))
        mv_slot_s[c] = jnp.where(((held >> target) & 1) == 1, w_slot_s[c], helped)
        return carry

    lax.fori_loop(0, DP, fill_help, 0)

    bits = helper_bits(me)
    lane = lax.broadcasted_iota(jnp.int32, (1, LANES), 1)
    able = (lane < DP) & (((bits >> (lane & 31)) & 1) == 1)
    helper_one = jnp.min(jnp.where(able, lane, DP - 1))
    helper_two = jnp.min(jnp.where(able & (lane > helper_one), lane, DP - 1))

    def slot_from(rank):
        x = (x0 - (rank >> 3)) & 3
        y = (y0 - ((rank >> 1) & 3)) & 3
        z = (z0 - (rank & 1)) & 1
        return (x * 8 + y * 2 + z - 1) & (DP - 1)

    def find_row(j, carry):
        row = jnp.max(jnp.where(dest_row == me * K + j, old_row, 0))
        owner = row >> 4
        in_second = owner == fail_b
        lost = (owner == fail_a) | in_second
        helper = jnp.where(in_second, helper_two, helper_one)
        block = jnp.where(in_second, 2 * K, K)
        owner_s[j] = slot_from(owner)
        sender_s[j] = jnp.where(lost & me_failed, slot_from(helper), DP)
        local_s[j] = jnp.where(lost & jnp.logical_not(me_failed), block + (row & 15), 0)
        lost_rows[pl.ds(j, 1), :] = jnp.broadcast_to(jnp.where(lost, 1.0, 0.0), (1, LANES))
        return carry

    lax.fori_loop(0, K, find_row, 0)

    loads[7].wait()
    for kind, rank in ((1, fail_a), (2, fail_b)):

        def store_lost(span, value, rows=pl.ds(kind * K, K)):
            mv_code[rows, span] = value

        code_block(
            lambda step, base=0, rank=rank: replica[rank, :, cols(step, base)].astype(jnp.float32),
            store_lost,
        )

    loads[8].wait()
    waiting(15, LANES, far_sem.at[1]).wait()
    grad_total = jnp.sum(
        part[1:2, :] + jnp.sum(far_parts[0:15, :], axis=0, keepdims=True), axis=1, keepdims=True
    )
    clip = jnp.minimum(1.0, lax.rsqrt(grad_total / float(DP * PIPE * K * D) + clip_eps))

    bound = scales[0:K, :] + clip * scales[K : 2 * K, :]
    to_unit = tiled(1.0 / bound)
    clip_scale = grad_scale * clip

    def code_moments(step, carry):
        here = cols(step)
        clipped = quant[:, here].astype(jnp.float32) * clip_scale
        first = (keep * beta_one) * moment1[:, here] + (1.0 - beta_one) * clipped
        second = (keep * beta_two) * moment2[:, here] + (1.0 - beta_two) * clipped * clipped
        root = jnp.sqrt(jnp.abs(first) * to_unit) * 32767.0
        high = nearest(jnp.where(first < 0.0, -root, root))
        level = (jnp.log2(jnp.maximum(second, 0.2)) - LOG_LOW) * LOG_UNIT
        low = nearest(jnp.clip(level, 0.0, 65535.0))
        mv_code[0:K, here] = (high << 16) | low
        return carry

    for piece, (base, width) in enumerate(zip(BASES, PIECES)):
        lax.fori_loop(base // WIDE, (base + width) // WIDE, code_moments, 0)
        span = pl.ds(base, width)

        def fill_mv(c, span=span):
            mv_send[pl.ds(c - 1, 1), span] = mv_code[pl.ds(mv_slot_s[c], 1), span]

        def send_mv(c, span=span, piece=piece):
            send(
                mv_send.at[pl.ds(c - 1, 1), span],
                mv_recvs[piece].at[pl.ds(c - 1, 1)],
                mv_sem.at[piece],
                device_at(c),
            )

        codes = [k * STRIDE % DP for k in range(1, DP)]
        fill_mv(codes[0])
        for before, c in zip(codes, codes[1:]):
            fill_mv(c)
            send_mv(before)
        send_mv(codes[-1])
        mv_recvs[piece][DP - 1 : DP, :] = mv_code[pl.ds(mv_slot_s[0], 1), span]

    waiting(DP - 1, W_COLS, w_sem.at[1]).wait()

    def place_scales(j, carry):
        w_rows[pl.ds(j, 1), HALF + LANES : W_COLS] = w_recv[
            pl.ds(owner_s[j], 1), HALF + LANES : W_COLS
        ]
        return carry

    lax.fori_loop(0, K, place_scales, 0)
    came_bound = scale_value(w_rows[:, HALF + LANES : HALF + 2 * LANES]) + clip * scale_value(
        w_rows[:, HALF + 2 * LANES : W_COLS]
    )
    from_unit = tiled(jnp.sqrt(came_bound) * (1.0 / 32767.0))
    row_lost = tiled(lost_rows[...]) > 0.5

    def place_w(j, carry):
        local = local_s[j]
        sender = sender_s[j]
        helped = sender < DP
        sender = jnp.minimum(sender, DP - 1)
        for piece in range(3):
            base = BASES[piece]
            width = min(PIECES[piece], HALF + LANES - base)
            span = pl.ds(base, max(width, 2 * LANES))
            from_peer = w_recv[pl.ds(owner_s[j], 1), span]
            from_here = mv_code[pl.ds(local, 1), span]
            from_helper = mv_recvs[piece][pl.ds(sender, 1), 0 : max(width, 2 * LANES)]
            words = jnp.where(helped, from_helper, jnp.where(local > 0, from_here, from_peer))
            w_rows[pl.ds(j, 1), span] = words
        return carry

    def take_w():
        lax.fori_loop(0, K, place_w, 0)
        w_unit = tiled(scale_value(w_rows[:, HALF : HALF + LANES]) * (1.0 / 32767.0))

        def decode_w(step, carry):
            word = w_rows[:, cols(step)]
            w_ref[:, cols(step)] = ((word << 16) >> 16).astype(jnp.float32) * w_unit
            w_ref[:, cols(step, HALF)] = (word >> 16).astype(jnp.float32) * w_unit
            return carry

        lax.fori_loop(0, HALF // WIDE, decode_w, 0)

    def decode_mv(step, carry):
        here = cols(step)
        word = mv_rows[:, here]
        signed_root = (word >> 16).astype(jnp.float32) * from_unit
        low = (word & 0xFFFF).astype(jnp.float32)
        grown = jnp.exp2(low * (0.5 / LOG_UNIT) + 0.5 * (LOG_LOW - math.log2(corr_two)))
        r_ref[:, here] = signed_root
        u_ref[:, here] = jnp.where(
            row_lost, signed_root * signed_root * math.sqrt(5.0 / corr_two), grown
        )
        return carry

    for piece, (base, width) in enumerate(zip(BASES, PIECES)):
        waiting(DP - 1, width, mv_sem.at[piece, 1]).wait()

        def place_mv(j, carry, piece=piece, base=base, width=width):
            mv_rows[pl.ds(j, 1), pl.ds(base, width)] = mv_recvs[piece][pl.ds(owner_s[j], 1), :]
            return carry

        lax.fori_loop(0, K, place_mv, 0)
        lax.fori_loop(base // WIDE, (base + width) // WIDE, decode_mv, 0)
        if piece == 2:
            take_w()

    waiting(7, LANES, near_sem.at[0]).wait()
    waiting(15, LANES, far_sem.at[0]).wait()
    waiting(DP - 1, W_COLS, w_sem.at[0]).wait()
    for piece, width in enumerate(PIECES):
        waiting(DP - 1, width, mv_sem.at[piece, 0]).wait()


def local(master, moment1, moment2, quant_grad, grad_exponent, replica_params, failed, dest):
    f32, i32 = jnp.float32, jnp.int32
    hbm = pl.BlockSpec(memory_space=pltpu.HBM)
    vmem = pl.BlockSpec(memory_space=pltpu.VMEM)
    dma = pltpu.SemaphoreType.DMA
    start, signed_root, root = pl.pallas_call(
        kernel,
        out_shape=(jax.ShapeDtypeStruct((K, D), f32),) * 3,
        in_specs=[hbm] * 8,
        out_specs=(vmem,) * 3,
        scratch_shapes=[
            pltpu.VMEM((K, D), f32),
            pltpu.VMEM((K, D), f32),
            pltpu.VMEM((K, D), f32),
            pltpu.VMEM((K, D), jnp.bfloat16),
            pltpu.VMEM((1, K), i32),
            pltpu.VMEM((DP, K, D), jnp.bfloat16),
            pltpu.VMEM((PIPE, DP * K), i32),
            pltpu.SMEM((2, PIPE), i32),
            pltpu.SMEM((PIPE, DP * K), i32),
            pltpu.VMEM((8, LANES), f32),
            pltpu.VMEM((8, LANES), f32),
            pltpu.VMEM((16, LANES), f32),
            pltpu.VMEM((K, W_COLS), i32),
            pltpu.VMEM((DP, W_COLS), i32),
            pltpu.VMEM((DP, W_COLS), i32),
            pltpu.VMEM((K, W_COLS), i32),
            pltpu.VMEM((3 * K, D), i32),
            pltpu.VMEM((DP, D), i32),
            [pltpu.VMEM((DP, width), i32) for width in PIECES],
            pltpu.VMEM((K, D), i32),
            pltpu.VMEM((2 * K, LANES), f32),
            pltpu.VMEM((K, LANES), f32),
            pltpu.VMEM((DP - 1, 1, W_COLS), i32),
            pltpu.SMEM((DP,), i32),
            pltpu.SMEM((DP,), i32),
            pltpu.SMEM((K,), i32),
            pltpu.SMEM((K,), i32),
            pltpu.SMEM((K,), i32),
            pltpu.SemaphoreType.REGULAR,
            pltpu.SemaphoreType.REGULAR,
            dma((9,)),
            dma((2,)),
            dma((2,)),
            dma((2,)),
            dma((len(PIECES), 2)),
        ],
        compiler_params=pltpu.CompilerParams(
            collective_id=0, has_side_effects=True, vmem_limit_bytes=24 * 2**20
        ),
        name="recover_step",
    )(
        *(
            pltpu.with_memory_space_constraint(x, pltpu.HBM)
            for x in (
                master[0],
                moment1[0],
                moment2[0],
                quant_grad[0],
                grad_exponent,
                replica_params[0, 0].reshape(DP, K, D),
                failed.T,
                dest,
            )
        )
    )
    first = signed_root * jnp.abs(signed_root)
    direction = first / corr_one / (root + adam_eps) + decay_rate * start
    return (
        (start - learn_rate * direction)[None],
        first[None],
        (corr_two * root * root)[None],
    )


def solution(mesh):
    in_specs = (
        P("pipe", "dp", None),
        P("pipe", "dp", None),
        P("pipe", "dp", None),
        P("pipe", "dp", None),
        P("pipe", "dp"),
        P("pipe", "dp", None, None),
        P(),
        P(),
    )
    out_specs = (P("pipe", "dp", None), P("pipe", "dp", None), P("pipe", "dp", None))
    return jax.shard_map(local, mesh=mesh, in_specs=in_specs, out_specs=out_specs, check_vma=False)
```

```python
import functools
import math

import jax
import jax.numpy as jnp
from jax import lax
from jax.experimental import pallas as pl
from jax.experimental.pallas import tpu as pltpu
from jax.sharding import PartitionSpec as P

STEP = 20

beta_one = 0.9
beta_two = 0.95
learn_rate = 0.00015
decay_rate = 0.1
adam_eps = 1e-08
clip_eps = 1e-06

corr_one = 1.0 - beta_one**STEP
corr_two = 1.0 - beta_two**STEP

LOGICAL = pl.DeviceIdType.LOGICAL
DP = 32
PIPE = 4
K = 16
D = 8192
HALF = D // 2
LANES = 128
W_COLS = HALF + 3 * LANES
PIECES = (2048, 2048, 2048, 1024, 1024)
BASES = tuple(sum(PIECES[:i]) for i in range(len(PIECES)))
WIDE = 1024
TILES = WIDE // LANES
STRIDE = 5

SCALE_UNIT = 65536.0
TINY = 1e-30
LOG_LOW = -2.2
LOG_SPAN = 16.0
LOG_UNIT = 65535.0 / LOG_SPAN


def cols(step, base=0):
    return pl.ds(pl.multiple_of(base + step * WIDE, LANES), WIDE)


def tiled(scale):
    return jnp.concatenate([scale] * TILES, axis=1)


def fold(acc, op):
    out = acc[:, :LANES]
    for t in range(1, TILES):
        out = op(out, acc[:, t * LANES : (t + 1) * LANES])
    return out


def scale_code(scale):
    return jnp.ceil(jnp.log2(jnp.maximum(scale, TINY)) * SCALE_UNIT).astype(jnp.int32)


def scale_value(code):
    return jnp.exp2(code.astype(jnp.float32) * (1.0 / SCALE_UNIT))


def nearest(x):
    return jnp.floor(x + 0.5).astype(jnp.int32)


def kernel(
    master_ref, moment1_ref, moment2_ref, quant_ref, expo_ref, replica_ref, failed_ref, dest_ref,
    w_ref, r_ref, u_ref,
    master, moment1, moment2, quant, expo, replica, dest_v, failed_s, dest_s,
    part, near_parts, far_parts, w_code, w_send, w_recv, w_rows, mv_code, mv_send, mv_recvs, mv_rows,
    scales, lost_rows, amount, w_slot_s, mv_slot_s, owner_s, sender_s, local_s,
    y_in, x_in, in_sem, near_sem, far_sem, w_sem, mv_sem,
):
    me = lax.axis_index("dp")
    group = lax.axis_index("pipe")

    def member(rank, section):
        return rank * PIPE + section

    x0, y0, z0 = lax.div(me, 8), lax.rem(lax.div(me, 2), 4), lax.rem(me, 2)

    def rank_at(c):
        x = lax.rem(x0 + c // 8, 4)
        y = lax.rem(y0 + (c // 2) % 4, 4)
        return x * 8 + y * 2 + lax.rem(z0 + c % 2, 2)

    x_parts = [lax.rem(x0 + d, 4) * (8 * PIPE) for d in range(4)]
    y_parts = [lax.rem(y0 + d, 4) * (2 * PIPE) for d in range(4)]
    z_parts = [lax.rem(z0 + d, 2) * PIPE + group for d in range(2)]

    def device_at(c):
        return x_parts[c // 8] + y_parts[(c // 2) % 4] + z_parts[c % 2]

    loads = [
        pltpu.make_async_copy(src, dst, in_sem.at[i])
        for i, (src, dst) in enumerate(
            (
                (quant_ref, quant),
                (expo_ref, expo),
                (dest_ref, dest_v),
                (dest_ref, dest_s),
                (failed_ref, failed_s),
                (master_ref, master),
                (moment1_ref, moment1),
                (replica_ref, replica),
                (moment2_ref, moment2),
            )
        )
    ]
    barrier = pltpu.get_barrier_semaphore()

    def greet(device):
        pl.semaphore_signal(barrier, inc=1, device_id=device, device_id_type=LOGICAL)

    flat = member(me, group)
    column = [flat // 8 * 8 + lax.rem(flat + q, 8) for q in range(1, 8)]
    along_y = [flat // 32 * 32 + lax.rem(flat + 8 * q, 32) for q in range(1, 4)]
    along_x = [lax.rem(flat + 32 * q, 128) for q in range(1, 4)]
    for device in (*column, *along_y, *along_x):
        greet(device)
    for load in loads[:7]:
        load.start()

    loads[0].wait()
    loads[1].wait()
    line = lax.broadcasted_iota(jnp.int32, (K, K), 0)
    place = lax.broadcasted_iota(jnp.int32, (K, K), 1)
    expo_rows = jnp.sum(
        jnp.where(line == place, jnp.broadcast_to(expo[...].astype(jnp.float32), (K, K)), 0.0),
        axis=1,
        keepdims=True,
    )
    grad_scale = jnp.exp2(expo_rows)

    def scan_grad(step, carry):
        total, largest = carry
        x = quant[:, cols(step)].astype(jnp.float32)
        return total + x * x, jnp.maximum(largest, jnp.abs(x))

    zero_step = jnp.zeros((K, WIDE), jnp.float32)
    total, largest = lax.fori_loop(0, D // WIDE, scan_grad, (zero_step, zero_step))
    squares = fold(total, jnp.add) * (grad_scale * grad_scale)
    part[0:1, :] = jnp.sum(squares, axis=0, keepdims=True)
    grad_code = scale_code(fold(largest, jnp.maximum) * ((1.0 - beta_one) * grad_scale))

    def waiting(slots, width, sem):
        held_bytes = amount.at[pl.ds(0, slots), :, pl.ds(0, width)]
        return pltpu.make_async_copy(held_bytes, held_bytes, sem)

    def send(src, dst, sems, device):
        pltpu.make_async_remote_copy(
            src_ref=src,
            dst_ref=dst,
            send_sem=sems.at[0],
            recv_sem=sems.at[1],
            device_id=device,
            device_id_type=LOGICAL,
        ).start()

    pl.semaphore_wait(barrier, 13)
    for q, device in enumerate(column):
        send(part.at[pl.ds(0, 1)], near_parts.at[pl.ds(q, 1)], near_sem, device)
    for device in (*along_y, device_at(1)):
        pl.semaphore_signal(y_in, inc=1, device_id=device, device_id_type=LOGICAL)

    for load in loads[2:5]:
        load.wait()
    fail_a = failed_s[0, group]
    fail_b = failed_s[1, group]
    me_failed = (me == fail_a) | (me == fail_b)

    held = jnp.int32(0)
    words = [jnp.int32(0)] * 4
    for i in range(K):
        target = dest_s[group, me * K + i] >> 4
        nibble = i << (4 * (target & 7))
        words = [word | jnp.where((target >> 3) == q, nibble, 0) for q, word in enumerate(words)]
        held = held | (1 << target)

    dest_row = dest_v[pl.ds(group, 1), :]
    old_row = lax.broadcasted_iota(jnp.int32, (1, DP * K), 1)
    old_rank = old_row >> 4
    new_rank = dest_row >> 4
    alive_bits = ~((1 << fail_a) | (1 << fail_b))

    def fill_slot(c, carry):
        target = rank_at(c)
        word = words[0]
        for q in range(1, 4):
            word = jnp.where((target >> 3) == q, words[q], word)
        w_slot_s[c] = (word >> (4 * (target & 7))) & 15
        return carry

    lax.fori_loop(0, DP, fill_slot, 0)

    loads[5].wait()
    loads[6].wait()
    loads[7].start()
    loads[8].start()

    def scan_moment(step, largest):
        return jnp.maximum(largest, jnp.abs(moment1[:, cols(step)]))

    keep = jnp.where(me_failed, 0.0, 1.0).astype(jnp.float32)
    largest = lax.fori_loop(0, D // WIDE, scan_moment, zero_step)
    moment_code = scale_code(fold(largest, jnp.maximum) * (keep * beta_one))
    scales[0:K, :] = scale_value(moment_code)
    scales[K : 2 * K, :] = scale_value(grad_code)
    w_code[:, HALF + LANES : HALF + 2 * LANES] = moment_code
    w_code[:, HALF + 2 * LANES : HALF + 3 * LANES] = grad_code

    def code_block(weights, store):
        def scan_weights(step, largest):
            return jnp.maximum(largest, jnp.abs(weights(step)))

        largest = lax.fori_loop(0, D // WIDE, scan_weights, zero_step)
        code = scale_code(fold(largest, jnp.maximum))
        to_code = tiled(32767.0 / scale_value(code))
        store(pl.ds(HALF, LANES), code)

        def code_weights(step, carry):
            low = nearest(weights(step) * to_code)
            high = nearest(weights(step, HALF) * to_code)
            store(cols(step), (high << 16) | (low & 0xFFFF))
            return carry

        lax.fori_loop(0, HALF // WIDE, code_weights, 0)

    def store_own(span, value):
        w_code[:, span] = value

    code_block(lambda step, base=0: master[:, cols(step, base)], store_own)

    def fill_w(c):
        w_send[pl.ds(c - 1, 1), :] = w_code[pl.ds(w_slot_s[c], 1), :]

    def send_w(c):
        send(
            w_send.at[pl.ds(c - 1, 1)],
            w_recv.at[pl.ds(c - 1, 1)],
            w_sem,
            device_at(c),
        )

    for c in (1, 2, 8, 6, 24, 4, 16):
        fill_w(c)
    for c in (1, 2, 8, 6, 24, 4, 16):
        send_w(c)

    pl.semaphore_wait(y_in, 4)
    for device in along_x:
        pl.semaphore_signal(x_in, inc=1, device_id=device, device_id_type=LOGICAL)

    def send_group(codes):
        fill_w(codes[0])
        for before, c in zip(codes, codes[1:]):
            fill_w(c)
            send_w(before)
        send_w(codes[-1])

    send_group([3, 18, 9, 12, 5, 26, 17, 10, 7, 20, 25, 28, 14, 22, 30])

    waiting(7, LANES, near_sem.at[1]).wait()
    part[1:2, :] = part[0:1, :] + jnp.sum(near_parts[0:7, :], axis=0, keepdims=True)
    for k in range(1, 16):
        q = (k * STRIDE) % 16
        send(
            part.at[pl.ds(1, 1)],
            far_parts.at[pl.ds(q - 1, 1)],
            far_sem,
            device_at(2 * q),
        )

    pl.semaphore_wait(x_in, 3)
    send_group([21, 11, 31, 13, 27, 23, 19, 15, 29])
    w_recv[DP - 1 : DP, :] = w_code[pl.ds(w_slot_s[0], 1), :]

    def helper_bits(receiver):
        bits = jnp.sum(jnp.where(new_rank == receiver, 1 << old_rank, 0))
        return alive_bits & ~bits

    def helper_row(receiver):
        bits = helper_bits(receiver)
        first = jnp.max(jnp.where((new_rank == receiver) & (old_rank == fail_a), old_row & 15, 0))
        second = jnp.max(jnp.where((new_rank == receiver) & (old_rank == fail_b), old_row & 15, 0))
        able = ((bits >> me) & 1) == 1
        lower = bits & ((1 << me) - 1)
        is_first = able & (lower == 0)
        is_second = able & (lower != 0) & ((lower & (lower - 1)) == 0)
        return jnp.where(is_first, K + first, jnp.where(is_second, 2 * K + second, 0))

    help_a = helper_row(fail_a)
    help_b = helper_row(fail_b)

    help_a = helper_row(fail_a)
    help_b = helper_row(fail_b)

    def fill_help(c, carry):
        target = rank_at(c)
        helped = jnp.where(target == fail_a, help_a, jnp.where(target == fail_b, help_b, 0))
        mv_slot_s[c] = jnp.where(((held >> target) & 1) == 1, w_slot_s[c], helped)
        return carry

    lax.fori_loop(0, DP, fill_help, 0)

    bits = helper_bits(me)
    lane = lax.broadcasted_iota(jnp.int32, (1, LANES), 1)
    able = (lane < DP) & (((bits >> (lane & 31)) & 1) == 1)
    helper_one = jnp.min(jnp.where(able, lane, DP - 1))
    helper_two = jnp.min(jnp.where(able & (lane > helper_one), lane, DP - 1))

    def slot_from(rank):
        x = (x0 - (rank >> 3)) & 3
        y = (y0 - ((rank >> 1) & 3)) & 3
        z = (z0 - (rank & 1)) & 1
        return (x * 8 + y * 2 + z - 1) & (DP - 1)

    def find_row(j, carry):
        row = jnp.max(jnp.where(dest_row == me * K + j, old_row, 0))
        owner = row >> 4
        in_second = owner == fail_b
        lost = (owner == fail_a) | in_second
        helper = jnp.where(in_second, helper_two, helper_one)
        block = jnp.where(in_second, 2 * K, K)
        owner_s[j] = slot_from(owner)
        sender_s[j] = jnp.where(lost & me_failed, slot_from(helper), DP)
        local_s[j] = jnp.where(lost & jnp.logical_not(me_failed), block + (row & 15), 0)
        lost_rows[pl.ds(j, 1), :] = jnp.broadcast_to(jnp.where(lost, 1.0, 0.0), (1, LANES))
        return carry

    lax.fori_loop(0, K, find_row, 0)

    loads[7].wait()
    for kind, rank in ((1, fail_a), (2, fail_b)):

        def store_lost(span, value, rows=pl.ds(kind * K, K)):
            mv_code[rows, span] = value

        code_block(
            lambda step, base=0, rank=rank: replica[rank, :, cols(step, base)].astype(jnp.float32),
            store_lost,
        )

    loads[8].wait()
    waiting(15, LANES, far_sem.at[1]).wait()
    grad_total = jnp.sum(
        part[1:2, :] + jnp.sum(far_parts[0:15, :], axis=0, keepdims=True), axis=1, keepdims=True
    )
    clip = jnp.minimum(1.0, lax.rsqrt(grad_total / float(DP * PIPE * K * D) + clip_eps))

    bound = scales[0:K, :] + clip * scales[K : 2 * K, :]
    to_unit = tiled(1.0 / bound)
    clip_scale = grad_scale * clip

    def code_moments(step, carry):
        here = cols(step)
        clipped = quant[:, here].astype(jnp.float32) * clip_scale
        first = (keep * beta_one) * moment1[:, here] + (1.0 - beta_one) * clipped
        second = (keep * beta_two) * moment2[:, here] + (1.0 - beta_two) * clipped * clipped
        root = jnp.sqrt(jnp.abs(first) * to_unit) * 32767.0
        high = nearest(jnp.where(first < 0.0, -root, root))
        level = (jnp.log2(jnp.maximum(second, 0.2)) - LOG_LOW) * LOG_UNIT
        low = nearest(jnp.clip(level, 0.0, 65535.0))
        mv_code[0:K, here] = (high << 16) | low
        return carry

    for piece, (base, width) in enumerate(zip(BASES, PIECES)):
        lax.fori_loop(base // WIDE, (base + width) // WIDE, code_moments, 0)
        span = pl.ds(base, width)

        def fill_mv(c, span=span):
            mv_send[pl.ds(c - 1, 1), span] = mv_code[pl.ds(mv_slot_s[c], 1), span]

        def send_mv(c, span=span, piece=piece):
            send(
                mv_send.at[pl.ds(c - 1, 1), span],
                mv_recvs[piece].at[pl.ds(c - 1, 1)],
                mv_sem.at[piece],
                device_at(c),
            )

        codes = [k * 27 % DP for k in range(1, DP)]
        fill_mv(codes[0])
        for before, c in zip(codes, codes[1:]):
            fill_mv(c)
            send_mv(before)
        send_mv(codes[-1])
        mv_recvs[piece][DP - 1 : DP, :] = mv_code[pl.ds(mv_slot_s[0], 1), span]

    waiting(DP - 1, W_COLS, w_sem.at[1]).wait()

    def place_scales(j, carry):
        w_rows[pl.ds(j, 1), HALF + LANES : W_COLS] = w_recv[
            pl.ds(owner_s[j], 1), HALF + LANES : W_COLS
        ]
        return carry

    lax.fori_loop(0, K, place_scales, 0)
    came_bound = scale_value(w_rows[:, HALF + LANES : HALF + 2 * LANES]) + clip * scale_value(
        w_rows[:, HALF + 2 * LANES : W_COLS]
    )
    from_unit = tiled(jnp.sqrt(came_bound) * (1.0 / 32767.0))
    row_lost = tiled(lost_rows[...]) > 0.5

    def place_w(j, carry):
        local = local_s[j]
        sender = sender_s[j]
        helped = sender < DP
        sender = jnp.minimum(sender, DP - 1)
        for piece in range(3):
            base = BASES[piece]
            width = min(PIECES[piece], HALF + LANES - base)
            span = pl.ds(base, max(width, 2 * LANES))
            from_peer = w_recv[pl.ds(owner_s[j], 1), span]
            from_here = mv_code[pl.ds(local, 1), span]
            from_helper = mv_recvs[piece][pl.ds(sender, 1), 0 : max(width, 2 * LANES)]
            words = jnp.where(helped, from_helper, jnp.where(local > 0, from_here, from_peer))
            w_rows[pl.ds(j, 1), span] = words
        return carry

    def take_w():
        lax.fori_loop(0, K, place_w, 0)
        w_unit = tiled(scale_value(w_rows[:, HALF : HALF + LANES]) * (1.0 / 32767.0))

        def decode_w(step, carry):
            word = w_rows[:, cols(step)]
            w_ref[:, cols(step)] = ((word << 16) >> 16).astype(jnp.float32) * w_unit
            w_ref[:, cols(step, HALF)] = (word >> 16).astype(jnp.float32) * w_unit
            return carry

        lax.fori_loop(0, HALF // WIDE, decode_w, 0)

    def decode_mv(step, carry):
        here = cols(step)
        word = mv_rows[:, here]
        signed_root = (word >> 16).astype(jnp.float32) * from_unit
        low = (word & 0xFFFF).astype(jnp.float32)
        grown = jnp.exp2(low * (0.5 / LOG_UNIT) + 0.5 * (LOG_LOW - math.log2(corr_two)))
        r_ref[:, here] = signed_root
        u_ref[:, here] = jnp.where(
            row_lost, signed_root * signed_root * math.sqrt(5.0 / corr_two), grown
        )
        return carry

    for piece, (base, width) in enumerate(zip(BASES, PIECES)):
        waiting(DP - 1, width, mv_sem.at[piece, 1]).wait()

        def place_mv(j, carry, piece=piece, base=base, width=width):
            mv_rows[pl.ds(j, 1), pl.ds(base, width)] = mv_recvs[piece][pl.ds(owner_s[j], 1), :]
            return carry

        lax.fori_loop(0, K, place_mv, 0)
        lax.fori_loop(base // WIDE, (base + width) // WIDE, decode_mv, 0)
        if piece == 2:
            take_w()

    waiting(7, LANES, near_sem.at[0]).wait()
    waiting(15, LANES, far_sem.at[0]).wait()
    waiting(DP - 1, W_COLS, w_sem.at[0]).wait()
    for piece, width in enumerate(PIECES):
        waiting(DP - 1, width, mv_sem.at[piece, 0]).wait()


def local(master, moment1, moment2, quant_grad, grad_exponent, replica_params, failed, dest):
    f32, i32 = jnp.float32, jnp.int32
    hbm = pl.BlockSpec(memory_space=pltpu.HBM)
    vmem = pl.BlockSpec(memory_space=pltpu.VMEM)
    dma = pltpu.SemaphoreType.DMA
    start, signed_root, root = pl.pallas_call(
        kernel,
        out_shape=(jax.ShapeDtypeStruct((K, D), f32),) * 3,
        in_specs=[hbm] * 8,
        out_specs=(vmem,) * 3,
        scratch_shapes=[
            pltpu.VMEM((K, D), f32),
            pltpu.VMEM((K, D), f32),
            pltpu.VMEM((K, D), f32),
            pltpu.VMEM((K, D), jnp.bfloat16),
            pltpu.VMEM((1, K), i32),
            pltpu.VMEM((DP, K, D), jnp.bfloat16),
            pltpu.VMEM((PIPE, DP * K), i32),
            pltpu.SMEM((2, PIPE), i32),
            pltpu.SMEM((PIPE, DP * K), i32),
            pltpu.VMEM((8, LANES), f32),
            pltpu.VMEM((8, LANES), f32),
            pltpu.VMEM((16, LANES), f32),
            pltpu.VMEM((K, W_COLS), i32),
            pltpu.VMEM((DP, W_COLS), i32),
            pltpu.VMEM((DP, W_COLS), i32),
            pltpu.VMEM((K, W_COLS), i32),
            pltpu.VMEM((3 * K, D), i32),
            pltpu.VMEM((DP, D), i32),
            [pltpu.VMEM((DP, width), i32) for width in PIECES],
            pltpu.VMEM((K, D), i32),
            pltpu.VMEM((2 * K, LANES), f32),
            pltpu.VMEM((K, LANES), f32),
            pltpu.VMEM((DP - 1, 1, W_COLS), i32),
            pltpu.SMEM((DP,), i32),
            pltpu.SMEM((DP,), i32),
            pltpu.SMEM((K,), i32),
            pltpu.SMEM((K,), i32),
            pltpu.SMEM((K,), i32),
            pltpu.SemaphoreType.REGULAR,
            pltpu.SemaphoreType.REGULAR,
            dma((9,)),
            dma((2,)),
            dma((2,)),
            dma((2,)),
            dma((len(PIECES), 2)),
        ],
        compiler_params=pltpu.CompilerParams(
            collective_id=0, has_side_effects=True, vmem_limit_bytes=24 * 2**20
        ),
        name="recover_step",
    )(
        *(
            pltpu.with_memory_space_constraint(x, pltpu.HBM)
            for x in (
                master[0],
                moment1[0],
                moment2[0],
                quant_grad[0],
                grad_exponent,
                replica_params[0, 0].reshape(DP, K, D),
                failed.T,
                dest,
            )
        )
    )
    first = signed_root * jnp.abs(signed_root)
    direction = first / corr_one / (root + adam_eps) + decay_rate * start
    return (
        (start - learn_rate * direction)[None],
        first[None],
        (corr_two * root * root)[None],
    )


def solution(mesh):
    in_specs = (
        P("pipe", "dp", None),
        P("pipe", "dp", None),
        P("pipe", "dp", None),
        P("pipe", "dp", None),
        P("pipe", "dp"),
        P("pipe", "dp", None, None),
        P(),
        P(),
    )
    out_specs = (P("pipe", "dp", None), P("pipe", "dp", None), P("pipe", "dp", None))
    return jax.shard_map(local, mesh=mesh, in_specs=in_specs, out_specs=out_specs, check_vma=False)
```

```python
import functools
import math

import jax
import jax.numpy as jnp
from jax import lax
from jax.experimental import pallas as pl
from jax.experimental.pallas import tpu as pltpu
from jax.sharding import PartitionSpec as P

STEP = 20

beta_one = 0.9
beta_two = 0.95
learn_rate = 0.00015
decay_rate = 0.1
adam_eps = 1e-08
clip_eps = 1e-06

corr_one = 1.0 - beta_one**STEP
corr_two = 1.0 - beta_two**STEP

LOGICAL = pl.DeviceIdType.LOGICAL
DP = 32
PIPE = 4
K = 16
D = 8192
HALF = D // 2
LANES = 128
W_COLS = HALF + 3 * LANES
PIECES = (2048, 2048, 2048, 1024, 1024)
BASES = tuple(sum(PIECES[:i]) for i in range(len(PIECES)))
WIDE = 1024
TILES = WIDE // LANES
STRIDE = 5

SCALE_UNIT = 65536.0
TINY = 1e-30
LOG_LOW = -2.2
LOG_SPAN = 16.0
LOG_UNIT = 65535.0 / LOG_SPAN


def cols(step, base=0):
    return pl.ds(pl.multiple_of(base + step * WIDE, LANES), WIDE)


def tiled(scale):
    return jnp.concatenate([scale] * TILES, axis=1)


def fold(acc, op):
    out = acc[:, :LANES]
    for t in range(1, TILES):
        out = op(out, acc[:, t * LANES : (t + 1) * LANES])
    return out


def scale_code(scale):
    return jnp.ceil(jnp.log2(jnp.maximum(scale, TINY)) * SCALE_UNIT).astype(jnp.int32)


def scale_value(code):
    return jnp.exp2(code.astype(jnp.float32) * (1.0 / SCALE_UNIT))


def nearest(x):
    return jnp.floor(x + 0.5).astype(jnp.int32)


def kernel(
    master_ref, moment1_ref, moment2_ref, quant_ref, expo_ref, replica_ref, failed_ref, dest_ref,
    w_ref, r_ref, u_ref,
    master, moment1, moment2, quant, expo, replica, dest_v, failed_s, dest_s,
    part, near_parts, far_parts, w_code, w_send, w_recv, w_rows, mv_code, mv_send, mv_recvs, mv_rows,
    scales, lost_rows, amount, w_slot_s, mv_slot_s, owner_s, sender_s, local_s,
    y_in, x_in, in_sem, near_sem, far_sem, w_sem, mv_sem,
):
    me = lax.axis_index("dp")
    group = lax.axis_index("pipe")

    def member(rank, section):
        return rank * PIPE + section

    x0, y0, z0 = lax.div(me, 8), lax.rem(lax.div(me, 2), 4), lax.rem(me, 2)

    def rank_at(c):
        x = lax.rem(x0 + c // 8, 4)
        y = lax.rem(y0 + (c // 2) % 4, 4)
        return x * 8 + y * 2 + lax.rem(z0 + c % 2, 2)

    x_parts = [lax.rem(x0 + d, 4) * (8 * PIPE) for d in range(4)]
    y_parts = [lax.rem(y0 + d, 4) * (2 * PIPE) for d in range(4)]
    z_parts = [lax.rem(z0 + d, 2) * PIPE + group for d in range(2)]

    def device_at(c):
        return x_parts[c // 8] + y_parts[(c // 2) % 4] + z_parts[c % 2]

    loads = [
        pltpu.make_async_copy(src, dst, in_sem.at[i])
        for i, (src, dst) in enumerate(
            (
                (quant_ref, quant),
                (expo_ref, expo),
                (dest_ref, dest_v),
                (dest_ref, dest_s),
                (failed_ref, failed_s),
                (master_ref, master),
                (moment1_ref, moment1),
                (replica_ref, replica),
                (moment2_ref, moment2),
            )
        )
    ]
    barrier = pltpu.get_barrier_semaphore()

    def greet(device):
        pl.semaphore_signal(barrier, inc=1, device_id=device, device_id_type=LOGICAL)

    flat = member(me, group)
    column = [flat // 8 * 8 + lax.rem(flat + q, 8) for q in range(1, 8)]
    along_y = [flat // 32 * 32 + lax.rem(flat + 8 * q, 32) for q in range(1, 4)]
    along_x = [lax.rem(flat + 32 * q, 128) for q in range(1, 4)]
    for device in (*column, *along_y, *along_x):
        greet(device)
    for load in loads[:7]:
        load.start()

    loads[0].wait()
    loads[1].wait()
    line = lax.broadcasted_iota(jnp.int32, (K, K), 0)
    place = lax.broadcasted_iota(jnp.int32, (K, K), 1)
    expo_rows = jnp.sum(
        jnp.where(line == place, jnp.broadcast_to(expo[...].astype(jnp.float32), (K, K)), 0.0),
        axis=1,
        keepdims=True,
    )
    grad_scale = jnp.exp2(expo_rows)

    def scan_grad(step, carry):
        total, largest = carry
        x = quant[:, cols(step)].astype(jnp.float32)
        return total + x * x, jnp.maximum(largest, jnp.abs(x))

    zero_step = jnp.zeros((K, WIDE), jnp.float32)
    total, largest = lax.fori_loop(0, D // WIDE, scan_grad, (zero_step, zero_step))
    squares = fold(total, jnp.add) * (grad_scale * grad_scale)
    part[0:1, :] = jnp.sum(squares, axis=0, keepdims=True)
    grad_code = scale_code(fold(largest, jnp.maximum) * ((1.0 - beta_one) * grad_scale))

    def waiting(slots, width, sem):
        held_bytes = amount.at[pl.ds(0, slots), :, pl.ds(0, width)]
        return pltpu.make_async_copy(held_bytes, held_bytes, sem)

    def send(src, dst, sems, device):
        pltpu.make_async_remote_copy(
            src_ref=src,
            dst_ref=dst,
            send_sem=sems.at[0],
            recv_sem=sems.at[1],
            device_id=device,
            device_id_type=LOGICAL,
        ).start()

    pl.semaphore_wait(barrier, 13)
    for q, device in enumerate(column):
        send(part.at[pl.ds(0, 1)], near_parts.at[pl.ds(q, 1)], near_sem, device)
    for device in (*along_y, device_at(1)):
        pl.semaphore_signal(y_in, inc=1, device_id=device, device_id_type=LOGICAL)

    for load in loads[2:5]:
        load.wait()
    fail_a = failed_s[0, group]
    fail_b = failed_s[1, group]
    me_failed = (me == fail_a) | (me == fail_b)

    held = jnp.int32(0)
    words = [jnp.int32(0)] * 4
    for i in range(K):
        target = dest_s[group, me * K + i] >> 4
        nibble = i << (4 * (target & 7))
        words = [word | jnp.where((target >> 3) == q, nibble, 0) for q, word in enumerate(words)]
        held = held | (1 << target)

    dest_row = dest_v[pl.ds(group, 1), :]
    old_row = lax.broadcasted_iota(jnp.int32, (1, DP * K), 1)
    old_rank = old_row >> 4
    new_rank = dest_row >> 4
    alive_bits = ~((1 << fail_a) | (1 << fail_b))

    def fill_slot(c, carry):
        target = rank_at(c)
        word = words[0]
        for q in range(1, 4):
            word = jnp.where((target >> 3) == q, words[q], word)
        w_slot_s[c] = (word >> (4 * (target & 7))) & 15
        return carry

    lax.fori_loop(0, DP, fill_slot, 0)

    loads[5].wait()
    loads[6].wait()

    def scan_moment(step, largest):
        return jnp.maximum(largest, jnp.abs(moment1[:, cols(step)]))

    keep = jnp.where(me_failed, 0.0, 1.0).astype(jnp.float32)
    largest = lax.fori_loop(0, D // WIDE, scan_moment, zero_step)
    moment_code = scale_code(fold(largest, jnp.maximum) * (keep * beta_one))
    scales[0:K, :] = scale_value(moment_code)
    scales[K : 2 * K, :] = scale_value(grad_code)
    w_code[:, HALF + LANES : HALF + 2 * LANES] = moment_code
    w_code[:, HALF + 2 * LANES : HALF + 3 * LANES] = grad_code

    def code_block(weights, store):
        def scan_weights(step, largest):
            return jnp.maximum(largest, jnp.abs(weights(step)))

        largest = lax.fori_loop(0, D // WIDE, scan_weights, zero_step)
        code = scale_code(fold(largest, jnp.maximum))
        to_code = tiled(32767.0 / scale_value(code))
        store(pl.ds(HALF, LANES), code)

        def code_weights(step, carry):
            low = nearest(weights(step) * to_code)
            high = nearest(weights(step, HALF) * to_code)
            store(cols(step), (high << 16) | (low & 0xFFFF))
            return carry

        lax.fori_loop(0, HALF // WIDE, code_weights, 0)

    def store_own(span, value):
        w_code[:, span] = value

    code_block(lambda step, base=0: master[:, cols(step, base)], store_own)

    def fill_w(c):
        w_send[pl.ds(c - 1, 1), :] = w_code[pl.ds(w_slot_s[c], 1), :]

    def send_w(c):
        send(
            w_send.at[pl.ds(c - 1, 1)],
            w_recv.at[pl.ds(c - 1, 1)],
            w_sem,
            device_at(c),
        )

    for c in (1, 2, 8, 6, 24, 4, 16):
        fill_w(c)
    for c in (1, 2, 8, 6, 24, 4, 16):
        send_w(c)

    pl.semaphore_wait(y_in, 4)
    for device in along_x:
        pl.semaphore_signal(x_in, inc=1, device_id=device, device_id_type=LOGICAL)

    def send_group(codes):
        fill_w(codes[0])
        for before, c in zip(codes, codes[1:]):
            fill_w(c)
            send_w(before)
        send_w(codes[-1])

    send_group([3, 18, 9, 12, 5, 26, 17, 10, 7, 20, 25, 28, 14, 22, 30])

    waiting(7, LANES, near_sem.at[1]).wait()
    part[1:2, :] = part[0:1, :] + jnp.sum(near_parts[0:7, :], axis=0, keepdims=True)
    for k in range(1, 16):
        q = (k * STRIDE) % 16
        send(
            part.at[pl.ds(1, 1)],
            far_parts.at[pl.ds(q - 1, 1)],
            far_sem,
            device_at(2 * q),
        )

    pl.semaphore_wait(x_in, 3)
    send_group([21, 11, 31, 13, 27, 23, 19, 15, 29])
    loads[8].start()
    loads[7].start()
    w_recv[DP - 1 : DP, :] = w_code[pl.ds(w_slot_s[0], 1), :]

    def helper_bits(receiver):
        bits = jnp.sum(jnp.where(new_rank == receiver, 1 << old_rank, 0))
        return alive_bits & ~bits

    def helper_row(receiver):
        bits = helper_bits(receiver)
        first = jnp.max(jnp.where((new_rank == receiver) & (old_rank == fail_a), old_row & 15, 0))
        second = jnp.max(jnp.where((new_rank == receiver) & (old_rank == fail_b), old_row & 15, 0))
        able = ((bits >> me) & 1) == 1
        lower = bits & ((1 << me) - 1)
        is_first = able & (lower == 0)
        is_second = able & (lower != 0) & ((lower & (lower - 1)) == 0)
        return jnp.where(is_first, K + first, jnp.where(is_second, 2 * K + second, 0))

    help_a = helper_row(fail_a)
    help_b = helper_row(fail_b)

    help_a = helper_row(fail_a)
    help_b = helper_row(fail_b)

    def fill_help(c, carry):
        target = rank_at(c)
        helped = jnp.where(target == fail_a, help_a, jnp.where(target == fail_b, help_b, 0))
        mv_slot_s[c] = jnp.where(((held >> target) & 1) == 1, w_slot_s[c], helped)
        return carry

    lax.fori_loop(0, DP, fill_help, 0)

    bits = helper_bits(me)
    lane = lax.broadcasted_iota(jnp.int32, (1, LANES), 1)
    able = (lane < DP) & (((bits >> (lane & 31)) & 1) == 1)
    helper_one = jnp.min(jnp.where(able, lane, DP - 1))
    helper_two = jnp.min(jnp.where(able & (lane > helper_one), lane, DP - 1))

    def slot_from(rank):
        x = (x0 - (rank >> 3)) & 3
        y = (y0 - ((rank >> 1) & 3)) & 3
        z = (z0 - (rank & 1)) & 1
        return (x * 8 + y * 2 + z - 1) & (DP - 1)

    def find_row(j, carry):
        row = jnp.max(jnp.where(dest_row == me * K + j, old_row, 0))
        owner = row >> 4
        in_second = owner == fail_b
        lost = (owner == fail_a) | in_second
        helper = jnp.where(in_second, helper_two, helper_one)
        block = jnp.where(in_second, 2 * K, K)
        owner_s[j] = slot_from(owner)
        sender_s[j] = jnp.where(lost & me_failed, slot_from(helper), DP)
        local_s[j] = jnp.where(lost & jnp.logical_not(me_failed), block + (row & 15), 0)
        lost_rows[pl.ds(j, 1), :] = jnp.broadcast_to(jnp.where(lost, 1.0, 0.0), (1, LANES))
        return carry

    lax.fori_loop(0, K, find_row, 0)

    loads[7].wait()
    for kind, rank in ((1, fail_a), (2, fail_b)):

        def store_lost(span, value, rows=pl.ds(kind * K, K)):
            mv_code[rows, span] = value

        code_block(
            lambda step, base=0, rank=rank: replica[rank, :, cols(step, base)].astype(jnp.float32),
            store_lost,
        )

    loads[8].wait()
    waiting(15, LANES, far_sem.at[1]).wait()
    grad_total = jnp.sum(
        part[1:2, :] + jnp.sum(far_parts[0:15, :], axis=0, keepdims=True), axis=1, keepdims=True
    )
    clip = jnp.minimum(1.0, lax.rsqrt(grad_total / float(DP * PIPE * K * D) + clip_eps))

    bound = scales[0:K, :] + clip * scales[K : 2 * K, :]
    to_unit = tiled(1.0 / bound)
    clip_scale = grad_scale * clip

    def code_moments(step, carry):
        here = cols(step)
        clipped = quant[:, here].astype(jnp.float32) * clip_scale
        first = (keep * beta_one) * moment1[:, here] + (1.0 - beta_one) * clipped
        second = (keep * beta_two) * moment2[:, here] + (1.0 - beta_two) * clipped * clipped
        root = jnp.sqrt(jnp.abs(first) * to_unit) * 32767.0
        high = nearest(jnp.where(first < 0.0, -root, root))
        level = (jnp.log2(jnp.maximum(second, 0.2)) - LOG_LOW) * LOG_UNIT
        low = nearest(jnp.clip(level, 0.0, 65535.0))
        mv_code[0:K, here] = (high << 16) | low
        return carry

    for piece, (base, width) in enumerate(zip(BASES, PIECES)):
        lax.fori_loop(base // WIDE, (base + width) // WIDE, code_moments, 0)
        span = pl.ds(base, width)

        def fill_mv(c, span=span):
            mv_send[pl.ds(c - 1, 1), span] = mv_code[pl.ds(mv_slot_s[c], 1), span]

        def send_mv(c, span=span, piece=piece):
            send(
                mv_send.at[pl.ds(c - 1, 1), span],
                mv_recvs[piece].at[pl.ds(c - 1, 1)],
                mv_sem.at[piece],
                device_at(c),
            )

        codes = [k * 27 % DP for k in range(1, DP)]
        fill_mv(codes[0])
        for before, c in zip(codes, codes[1:]):
            fill_mv(c)
            send_mv(before)
        send_mv(codes[-1])
        mv_recvs[piece][DP - 1 : DP, :] = mv_code[pl.ds(mv_slot_s[0], 1), span]

    waiting(DP - 1, W_COLS, w_sem.at[1]).wait()

    def place_scales(j, carry):
        w_rows[pl.ds(j, 1), HALF + LANES : W_COLS] = w_recv[
            pl.ds(owner_s[j], 1), HALF + LANES : W_COLS
        ]
        return carry

    lax.fori_loop(0, K, place_scales, 0)
    came_bound = scale_value(w_rows[:, HALF + LANES : HALF + 2 * LANES]) + clip * scale_value(
        w_rows[:, HALF + 2 * LANES : W_COLS]
    )
    from_unit = tiled(jnp.sqrt(came_bound) * (1.0 / 32767.0))
    row_lost = tiled(lost_rows[...]) > 0.5

    def place_w(j, carry):
        local = local_s[j]
        sender = sender_s[j]
        helped = sender < DP
        sender = jnp.minimum(sender, DP - 1)
        for piece in range(3):
            base = BASES[piece]
            width = min(PIECES[piece], HALF + LANES - base)
            span = pl.ds(base, max(width, 2 * LANES))
            from_peer = w_recv[pl.ds(owner_s[j], 1), span]
            from_here = mv_code[pl.ds(local, 1), span]
            from_helper = mv_recvs[piece][pl.ds(sender, 1), 0 : max(width, 2 * LANES)]
            words = jnp.where(helped, from_helper, jnp.where(local > 0, from_here, from_peer))
            w_rows[pl.ds(j, 1), span] = words
        return carry

    def take_w():
        lax.fori_loop(0, K, place_w, 0)
        w_unit = tiled(scale_value(w_rows[:, HALF : HALF + LANES]) * (1.0 / 32767.0))

        def decode_w(step, carry):
            word = w_rows[:, cols(step)]
            w_ref[:, cols(step)] = ((word << 16) >> 16).astype(jnp.float32) * w_unit
            w_ref[:, cols(step, HALF)] = (word >> 16).astype(jnp.float32) * w_unit
            return carry

        lax.fori_loop(0, HALF // WIDE, decode_w, 0)

    def decode_mv(step, carry):
        here = cols(step)
        word = mv_rows[:, here]
        signed_root = (word >> 16).astype(jnp.float32) * from_unit
        low = (word & 0xFFFF).astype(jnp.float32)
        grown = jnp.exp2(low * (0.5 / LOG_UNIT) + 0.5 * (LOG_LOW - math.log2(corr_two)))
        r_ref[:, here] = signed_root
        u_ref[:, here] = jnp.where(
            row_lost, signed_root * signed_root * math.sqrt(5.0 / corr_two), grown
        )
        return carry

    for piece, (base, width) in enumerate(zip(BASES, PIECES)):
        waiting(DP - 1, width, mv_sem.at[piece, 1]).wait()

        def place_mv(j, carry, piece=piece, base=base, width=width):
            mv_rows[pl.ds(j, 1), pl.ds(base, width)] = mv_recvs[piece][pl.ds(owner_s[j], 1), :]
            return carry

        lax.fori_loop(0, K, place_mv, 0)
        lax.fori_loop(base // WIDE, (base + width) // WIDE, decode_mv, 0)
        if piece == 2:
            take_w()

    waiting(7, LANES, near_sem.at[0]).wait()
    waiting(15, LANES, far_sem.at[0]).wait()
    waiting(DP - 1, W_COLS, w_sem.at[0]).wait()
    for piece, width in enumerate(PIECES):
        waiting(DP - 1, width, mv_sem.at[piece, 0]).wait()


def local(master, moment1, moment2, quant_grad, grad_exponent, replica_params, failed, dest):
    f32, i32 = jnp.float32, jnp.int32
    hbm = pl.BlockSpec(memory_space=pltpu.HBM)
    vmem = pl.BlockSpec(memory_space=pltpu.VMEM)
    dma = pltpu.SemaphoreType.DMA
    start, signed_root, root = pl.pallas_call(
        kernel,
        out_shape=(jax.ShapeDtypeStruct((K, D), f32),) * 3,
        in_specs=[hbm] * 8,
        out_specs=(vmem,) * 3,
        scratch_shapes=[
            pltpu.VMEM((K, D), f32),
            pltpu.VMEM((K, D), f32),
            pltpu.VMEM((K, D), f32),
            pltpu.VMEM((K, D), jnp.bfloat16),
            pltpu.VMEM((1, K), i32),
            pltpu.VMEM((DP, K, D), jnp.bfloat16),
            pltpu.VMEM((PIPE, DP * K), i32),
            pltpu.SMEM((2, PIPE), i32),
            pltpu.SMEM((PIPE, DP * K), i32),
            pltpu.VMEM((8, LANES), f32),
            pltpu.VMEM((8, LANES), f32),
            pltpu.VMEM((16, LANES), f32),
            pltpu.VMEM((K, W_COLS), i32),
            pltpu.VMEM((DP, W_COLS), i32),
            pltpu.VMEM((DP, W_COLS), i32),
            pltpu.VMEM((K, W_COLS), i32),
            pltpu.VMEM((3 * K, D), i32),
            pltpu.VMEM((DP, D), i32),
            [pltpu.VMEM((DP, width), i32) for width in PIECES],
            pltpu.VMEM((K, D), i32),
            pltpu.VMEM((2 * K, LANES), f32),
            pltpu.VMEM((K, LANES), f32),
            pltpu.VMEM((DP - 1, 1, W_COLS), i32),
            pltpu.SMEM((DP,), i32),
            pltpu.SMEM((DP,), i32),
            pltpu.SMEM((K,), i32),
            pltpu.SMEM((K,), i32),
            pltpu.SMEM((K,), i32),
            pltpu.SemaphoreType.REGULAR,
            pltpu.SemaphoreType.REGULAR,
            dma((9,)),
            dma((2,)),
            dma((2,)),
            dma((2,)),
            dma((len(PIECES), 2)),
        ],
        compiler_params=pltpu.CompilerParams(
            collective_id=0, has_side_effects=True, vmem_limit_bytes=24 * 2**20
        ),
        name="recover_step",
    )(
        *(
            pltpu.with_memory_space_constraint(x, pltpu.HBM)
            for x in (
                master[0],
                moment1[0],
                moment2[0],
                quant_grad[0],
                grad_exponent,
                replica_params[0, 0].reshape(DP, K, D),
                failed.T,
                dest,
            )
        )
    )
    first = signed_root * jnp.abs(signed_root)
    direction = first / corr_one / (root + adam_eps) + decay_rate * start
    return (
        (start - learn_rate * direction)[None],
        first[None],
        (corr_two * root * root)[None],
    )


def solution(mesh):
    in_specs = (
        P("pipe", "dp", None),
        P("pipe", "dp", None),
        P("pipe", "dp", None),
        P("pipe", "dp", None),
        P("pipe", "dp"),
        P("pipe", "dp", None, None),
        P(),
        P(),
    )
    out_specs = (P("pipe", "dp", None), P("pipe", "dp", None), P("pipe", "dp", None))
    return jax.shard_map(local, mesh=mesh, in_specs=in_specs, out_specs=out_specs, check_vma=False)
```
